32 devices in a mesh: dp: 8 (over z, x), mp: 4 (over y, core).
Axes of the slice: x: 2, y: 2, z: 4, core: 2. Of those that a mesh axis runs over, the one named last changes fastest.
Arguments:
- grad_tiles: bfloat16 [16, 512, 512], P(None, 'dp', 'mp'), may hold values from -8 to 8
- factor_stats: float32 [16, 2, 512, 512], P('dp', None, 'mp'), may hold values from -80 to 500, as said below
- owner_blocks: int32 [8, 2], replicated, may hold values from 0 to 15, as said below
- rotation: int32 [1], replicated, may hold values from 0 to 7
Outputs:
- preconditioned: bfloat16 [16, 512, 512], P(None, 'dp', 'mp')
- new_stats: float32 [16, 2, 512, 512], P('dp', None, 'mp')
The draws below stay inside these ranges and needn't reach their ends.
Inputs may be any that keep to these rules, and one draw needn't show every extreme that they name: Each matrix factor_stats[slot, side] is symmetric and positive definite. `owner_blocks`: every block number 0 to 15 stands exactly once.
All inputs are finite; a program needn't handle non-finite values.
Results may differ from the reference program's by a relative error of at most 0.0092.
Values may be sent and summed in bfloat16 or wider, within the bound.
No kernel may reach another device: no remote copies, remote signals or barrier semaphores. Data moves between devices by JAX's collectives and lax.ppermute only.
A program may use at most 64 MiB of HBM per device.

```python
import jax
import jax.numpy as jnp
from jax import lax

B = 512
CAP = 2
ITERS = 2
NBLK = 16
N_DP = 8


def draw_grad_tiles(key, part):
    key_noise = jax.random.fold_in(key, 11)
    key_rows = jax.random.fold_in(key, 12)
    base_noise = jax.random.normal(key_noise, (NBLK, B, B), jnp.float32)
    block_scale = jnp.exp(jax.random.uniform(key_rows, (NBLK, 1, 1), jnp.float32, jnp.log(0.5), jnp.log(2.0)))
    values = base_noise * block_scale
    return jnp.clip(values, -8.0, 8.0).astype(jnp.bfloat16)


def draw_factor_stats(key, part):
    key_noise = jax.random.fold_in(key, 21)
    key_diag = jax.random.fold_in(key, 22)
    slot_total = N_DP * CAP
    mixing = jnp.clip(jax.random.normal(key_noise, (slot_total, 2, B, B), jnp.float32), -4.0, 4.0)
    weight_scale = 0.35
    diagonal = jnp.exp(jax.random.uniform(key_diag, (slot_total, 2, B), jnp.float32, jnp.log(5.0), jnp.log(100.0)))
    accumulated = jnp.einsum('sgik,sgjk->sgij', mixing, mixing, precision=lax.Precision.HIGHEST)
    accumulated = 0.5 * (accumulated + jnp.swapaxes(accumulated, -1, -2))
    identity = jnp.eye(B, dtype=jnp.float32)
    return weight_scale * accumulated + identity * diagonal[..., None]


def draw_owner_blocks(key, part):
    key_perm = jax.random.fold_in(key, 31)
    block_ids = jax.random.permutation(key_perm, NBLK).astype(jnp.int32)
    return block_ids.reshape(N_DP, CAP).astype(jnp.int32)


def setup_inputs(seed: int = 0) -> dict:
    key_of = jax.random.split(jax.random.key(seed), 5)
    grad_tiles = draw_grad_tiles(jax.random.fold_in(key_of[4], 71), 0)
    factor_stats = draw_factor_stats(jax.random.fold_in(key_of[4], 71), 0)
    owner_blocks = draw_owner_blocks(jax.random.fold_in(key_of[4], 71), 0)
    rotation = jax.random.randint(key_of[3], (1,), 0, N_DP).astype(jnp.int32)
    return dict(grad_tiles=grad_tiles, factor_stats=factor_stats, owner_blocks=owner_blocks, rotation=rotation)


decay_rate = 0.9
damping = 1.0

def newton_root(factor):
    order = factor.shape[-1]
    identity = jnp.eye(order, dtype=jnp.float32)
    squares = jnp.sum(jnp.square(factor.astype(jnp.float32)))
    norm_scale = 2.5 / jnp.sqrt(squares)
    moment = (norm_scale * factor.astype(jnp.float32)).astype(jnp.bfloat16)
    current = None
    for newton_step in range(ITERS):
        step_t = ((5.0 * identity - moment.astype(jnp.float32)) * 0.25).astype(jnp.bfloat16)
        if newton_step == 0:
            current = step_t
        else:
            current = jnp.dot(current, step_t, preferred_element_type=jnp.float32).astype(jnp.bfloat16)
        if newton_step + 1 < ITERS:
            square = jnp.dot(step_t, step_t, preferred_element_type=jnp.float32).astype(jnp.bfloat16)
            partial_m = jnp.dot(square, moment, preferred_element_type=jnp.float32).astype(jnp.bfloat16)
            moment = jnp.dot(square, partial_m, preferred_element_type=jnp.float32).astype(jnp.bfloat16)
    return current

def one_block(inputs):
    grad_block, old_state = inputs
    identity = jnp.eye(grad_block.shape[0], dtype=jnp.float32)
    left_gram = jnp.dot(grad_block, grad_block.T, preferred_element_type=jnp.float32)
    right_gram = jnp.dot(grad_block.T, grad_block, preferred_element_type=jnp.float32)
    updated = decay_rate * old_state + (1.0 - decay_rate) * jnp.stack([left_gram, right_gram])
    factor = (updated + damping * identity).astype(jnp.bfloat16)
    left_root = newton_root(factor[0])
    right_root = newton_root(factor[1])
    right_applied = jnp.dot(grad_block, right_root, preferred_element_type=jnp.float32).astype(jnp.bfloat16)
    result = jnp.dot(left_root, right_applied, preferred_element_type=jnp.float32).astype(jnp.bfloat16)
    grad_norm = jnp.sqrt(jnp.sum(jnp.square(grad_block.astype(jnp.float32))))
    result_norm = jnp.sqrt(jnp.sum(jnp.square(result.astype(jnp.float32))))
    grafted = (result.astype(jnp.float32) * (grad_norm / (result_norm + 1e-06))).astype(jnp.bfloat16)
    return (updated, grafted)

def reference(grad_tiles, factor_stats, owner_blocks, rotation):
    owners = jnp.roll(owner_blocks, rotation[0], axis=0)
    owner_flat = owners.reshape(-1).astype(jnp.int32)
    slot_total = owner_flat.shape[0]
    position = jnp.zeros((NBLK,), jnp.int32).at[owner_flat].set(jnp.arange(slot_total, dtype=jnp.int32))
    own_stats = factor_stats[position]
    updated, preconditioned = lax.map(one_block, (grad_tiles, own_stats))
    new_stats = (decay_rate * factor_stats).at[position].set(updated)
    return (preconditioned, new_stats)
```

```python
import functools

import jax
import jax.numpy as jnp
from jax import lax
from jax.experimental import pallas as pl
from jax.experimental.pallas import tpu as pltpu
from jax.sharding import PartitionSpec as P

ITERS = 2


decay_rate = 0.9
damping = 1.0
bf16 = jnp.bfloat16
f32 = jnp.float32

VMEM = pl.BlockSpec(memory_space=pltpu.VMEM)
SMEM = pl.BlockSpec(memory_space=pltpu.SMEM)


def owner_of(owners_ref, rot, o, s, dp_count):
    row = o - rot
    return owners_ref[s, jnp.where(row < 0, row + dp_count, row)]


def pick_kernel(owners_ref, rot_ref, tiles_ref, out_ref, *, dp_count, slots):
    rot = rot_ref[0]

    def one(j, carry):
        out_ref[j] = tiles_ref[owner_of(owners_ref, rot, j // slots, j % slots, dp_count)]
        return carry

    lax.fori_loop(0, dp_count * slots, one, 0, unroll=dp_count * slots <= 16)


def place_kernel(owners_ref, rot_ref, in_ref, out_ref, *, dp_count, slots):
    rot = rot_ref[0]

    def one(j, carry):
        out_ref[owner_of(owners_ref, rot, j // slots, j % slots, dp_count)] = in_ref[j]
        return carry

    lax.fori_loop(0, dp_count * slots, one, 0, unroll=dp_count * slots <= 16)


def dot(a, b, dims=(((1,), (0,)), ((), ()))):
    return lax.dot_general(a, b, dims, preferred_element_type=f32)


def newton_root(factor, eye5):
    norm = jnp.sum(jnp.square(factor.astype(f32)))
    moment = (2.5 / jnp.sqrt(norm) * factor.astype(f32)).astype(bf16)
    current = None
    for newton_step in range(ITERS):
        step_t = ((eye5 - moment.astype(f32)) * 0.25).astype(bf16)
        current = step_t if newton_step == 0 else dot(current, step_t).astype(bf16)
        if newton_step + 1 < ITERS:
            square = dot(step_t, step_t).astype(bf16)
            partial_m = dot(square, moment).astype(bf16)
            moment = dot(square, partial_m).astype(bf16)
    return current


def owner_kernel(*refs, n_g, n_s, dp_count, mp_count, slots, piece_rows, tile_cols, split):
    meta_ref, refs = refs[0], refs[1:]
    g_refs, refs = refs[:n_g], refs[n_g:]
    s_refs, refs = refs[:n_s], refs[n_s:]
    own_ref, out_ref, send_ref, new_ref, g_scr, s_scr, gram_scr, res_scr = refs
    order = g_scr.shape[0]
    rows = own_ref.shape[1]
    tile_rows = order // dp_count
    parts = mp_count // slots
    if split:
        for k, g_ref in enumerate(g_refs):
            at = pl.multiple_of(meta_ref[1 + k], piece_rows)
            for o in range(dp_count):
                for m in range(mp_count):
                    g_scr[pl.ds(o * tile_rows + at, piece_rows), m * tile_cols : (m + 1) * tile_cols] = g_ref[
                        o * mp_count + m
                    ]
    else:
        g_scr[...] = g_refs[0][...]
    for k, s_ref in enumerate(s_refs):
        at = pl.multiple_of(meta_ref[1 + parts + k], rows)
        s_scr[:, pl.ds(at, rows), :] = s_ref[...]
    own_at = pl.multiple_of(meta_ref[1 + parts + mp_count + slots - 1], rows)
    ids = lax.broadcasted_iota(jnp.int32, (order, order), 0)
    eye = ids == lax.broadcasted_iota(jnp.int32, (order, order), 1)
    roots = []
    for side in range(2):
        grad = g_scr[...]
        across = 1 - side
        gram_scr[side] = dot(grad, grad, (((across,), (across,)), ((), ())))
        for k in range(slots - 1):
            at = pl.multiple_of(meta_ref[1 + parts + mp_count + k], rows)
            send_ref[k, side] = gram_scr[side, pl.ds(at, rows), :].astype(bf16)
        new_ref[side] = decay_rate * own_ref[side] + (1.0 - decay_rate) * gram_scr[side, pl.ds(own_at, rows), :]
        updated = decay_rate * s_scr[side].astype(f32) + (1.0 - decay_rate) * gram_scr[side]
        factor = (updated + jnp.where(eye, damping, 0.0)).astype(bf16)
        roots.append(newton_root(factor, jnp.where(eye, 5.0, 0.0)))
    right_applied = dot(g_scr[...], roots[1]).astype(bf16)
    result = dot(roots[0], right_applied).astype(bf16).astype(f32)
    grad_norm = jnp.sqrt(jnp.sum(jnp.square(g_scr[...].astype(f32))))
    result_norm = jnp.sqrt(jnp.sum(jnp.square(result)))
    res_scr[...] = (result * (grad_norm / (result_norm + 1e-06))).astype(bf16)
    if split:
        at = pl.multiple_of(meta_ref[0] * piece_rows, piece_rows)
        for o in range(dp_count):
            for m in range(mp_count):
                out_ref[o * mp_count + m] = res_scr[
                    pl.ds(o * tile_rows + at, piece_rows), m * tile_cols : (m + 1) * tile_cols
                ]
    else:
        out_ref[...] = res_scr[...]


def body(grad_tiles, factor_stats, owner_blocks, rotation):
    dp_count = lax.axis_size("dp")
    mp_count = lax.axis_size("mp")
    block_count, tile_rows, tile_cols = grad_tiles.shape
    slots = owner_blocks.shape[1]
    rows, order = factor_stats.shape[2:]
    parts = mp_count // slots
    piece_rows = tile_rows // parts
    split = piece_rows % 16 == 0 and tile_cols % 128 == 0
    my_index = lax.axis_index("mp")
    my_slot = my_index // parts
    my_part = my_index % parts
    owners = owner_blocks.T
    sizes = dict(dp_count=dp_count, slots=slots)

    def to_slot(x, ahead):
        return lax.ppermute(x, "mp", [(i, (i + ahead * parts) % mp_count) for i in range(mp_count)])

    def to_part(x, ahead):
        return lax.ppermute(
            x, "mp", [(i, i // parts * parts + (i + ahead) % parts) for i in range(mp_count)]
        )

    def slot_stats(ahead):
        return lax.dynamic_index_in_dim(factor_stats, (my_slot + ahead) % slots, 0, keepdims=False)

    chunks = [slot_stats(0).astype(bf16)]
    chunk_of = [my_index]
    for ahead in range(1, slots):
        chunks.append(to_slot(slot_stats(ahead).astype(bf16), ahead))
        chunk_of.append((my_slot - ahead) % slots * parts + my_part)
    for ahead in range(1, parts):
        for k in range(slots):
            chunks.append(to_part(chunks[k], ahead))
            chunk_of.append(chunk_of[k] // parts * parts + (my_part - ahead) % parts)

    picked = pl.pallas_call(
        functools.partial(pick_kernel, **sizes),
        out_shape=jax.ShapeDtypeStruct(grad_tiles.shape, bf16),
        in_specs=[SMEM, SMEM, VMEM],
        out_specs=VMEM,
    )(owners, rotation, grad_tiles)
    outgoing = picked.reshape(dp_count * mp_count, piece_rows, tile_cols)
    arrived = lax.all_to_all(outgoing, ("dp", "mp"), split_axis=0, concat_axis=0, tiled=True)
    pieces = [arrived] + [to_part(arrived, ahead) for ahead in range(1, parts)]
    if not split:
        held = jnp.take(jnp.stack(pieces), (my_part - jnp.arange(parts)) % parts, axis=0)
        held = held.reshape(parts, dp_count, mp_count, piece_rows, tile_cols)
        pieces = [held.transpose(1, 0, 3, 2, 4).reshape(order, order)]

    meta = jnp.stack(
        [my_part]
        + [(my_part - k) % parts * piece_rows for k in range(parts)]
        + [c * rows for c in chunk_of]
        + [((my_slot + k) % slots * parts + my_part) * rows for k in range(1, slots)]
        + [my_index * rows]
    ).astype(jnp.int32)
    result_shape = (dp_count * mp_count, piece_rows, tile_cols) if split else (order, order)
    result, gram_rows, own_rows = pl.pallas_call(
        functools.partial(
            owner_kernel,
            n_g=len(pieces),
            n_s=len(chunks),
            mp_count=mp_count,
            piece_rows=piece_rows,
            tile_cols=tile_cols,
            split=split,
            **sizes,
        ),
        out_shape=(
            jax.ShapeDtypeStruct(result_shape, bf16),
            jax.ShapeDtypeStruct((slots - 1, 2, rows, order), bf16),
            jax.ShapeDtypeStruct((2, rows, order), f32),
        ),
        in_specs=[SMEM] + [VMEM] * (len(pieces) + len(chunks) + 1),
        out_specs=(VMEM, VMEM, VMEM),
        scratch_shapes=[
            pltpu.VMEM((order, order), bf16),
            pltpu.VMEM((2, order, order), bf16),
            pltpu.VMEM((2, order, order), f32),
            pltpu.VMEM((order, order), bf16),
        ],
    )(meta, *pieces, *chunks, slot_stats(0))
    if not split:
        result = result.reshape(dp_count, parts, piece_rows, mp_count, tile_cols)
        result = lax.dynamic_index_in_dim(result, my_part, 1, keepdims=False)
        result = result.transpose(0, 2, 1, 3).reshape(dp_count * mp_count, piece_rows, tile_cols)

    stats_rows = [own_rows]
    for ahead in range(1, slots):
        theirs = to_slot(gram_rows[ahead - 1], ahead).astype(f32)
        stats_rows.append(decay_rate * slot_stats(-ahead) + (1.0 - decay_rate) * theirs)
    if slots == 2:
        new_stats = jnp.stack(
            [jnp.where(my_slot == s, stats_rows[0], stats_rows[1]) for s in range(2)]
        )
    else:
        new_stats = jnp.take(jnp.stack(stats_rows), (my_slot - jnp.arange(slots)) % slots, axis=0)

    returned = lax.all_to_all(result, ("dp", "mp"), split_axis=0, concat_axis=0, tiled=True)
    preconditioned = pl.pallas_call(
        functools.partial(place_kernel, **sizes),
        out_shape=jax.ShapeDtypeStruct(grad_tiles.shape, bf16),
        in_specs=[SMEM, SMEM, VMEM],
        out_specs=VMEM,
    )(owners, rotation, returned.reshape(grad_tiles.shape))
    return (preconditioned, new_stats)


def solution(mesh):
    return jax.shard_map(
        body,
        mesh=mesh,
        in_specs=(P(None, "dp", "mp"), P("dp", None, "mp", None), P(), P()),
        out_specs=(P(None, "dp", "mp"), P("dp", None, "mp", None)),
        check_vma=False,
    )
```

```python
import functools

import jax
import jax.numpy as jnp
from jax import lax
from jax.experimental import pallas as pl
from jax.experimental.pallas import tpu as pltpu
from jax.sharding import PartitionSpec as P

ITERS = 2


decay_rate = 0.9
damping = 1.0
bf16 = jnp.bfloat16
f32 = jnp.float32

VMEM = pl.BlockSpec(memory_space=pltpu.VMEM)
SMEM = pl.BlockSpec(memory_space=pltpu.SMEM)


def owner_of(owners_ref, rot, o, s, dp_count):
    row = o - rot
    return owners_ref[s, jnp.where(row < 0, row + dp_count, row)]


def pick_kernel(owners_ref, rot_ref, tiles_ref, out_ref, *, dp_count, slots):
    rot = rot_ref[0]

    def one(j, carry):
        out_ref[j] = tiles_ref[owner_of(owners_ref, rot, j // slots, j % slots, dp_count)]
        return carry

    lax.fori_loop(0, dp_count * slots, one, 0, unroll=dp_count * slots <= 16)


def place_kernel(owners_ref, rot_ref, in_ref, out_ref, *, dp_count, slots):
    rot = rot_ref[0]

    def one(j, carry):
        out_ref[owner_of(owners_ref, rot, j // slots, j % slots, dp_count)] = in_ref[j]
        return carry

    lax.fori_loop(0, dp_count * slots, one, 0, unroll=dp_count * slots <= 16)


def dot(a, b, dims=(((1,), (0,)), ((), ()))):
    return lax.dot_general(a, b, dims, preferred_element_type=f32)


def newton_root(factor, eye5):
    norm = jnp.sum(jnp.square(factor.astype(f32)))
    moment = (2.5 / jnp.sqrt(norm) * factor.astype(f32)).astype(bf16)
    current = None
    for newton_step in range(ITERS):
        step_t = ((eye5 - moment.astype(f32)) * 0.25).astype(bf16)
        current = step_t if newton_step == 0 else dot(current, step_t).astype(bf16)
        if newton_step + 1 < ITERS:
            square = dot(step_t, step_t).astype(bf16)
            partial_m = dot(square, moment).astype(bf16)
            moment = dot(square, partial_m).astype(bf16)
    return current


def gather_grad(g_refs, g_scr, part, *, dp_count, mp_count, parts, piece_rows, tile_cols):
    for k, g_ref in enumerate(g_refs):
        piece = part - k
        at = pl.multiple_of(jnp.where(piece < 0, piece + parts, piece) * piece_rows, piece_rows)
        for o in range(dp_count):
            for m in range(mp_count):
                rows = pl.ds(o * parts * piece_rows + at, piece_rows)
                g_scr[rows, m * tile_cols : (m + 1) * tile_cols] = g_ref[o * mp_count + m]


def owner_kernel(*refs, n_g, split, sizes):
    g_refs, refs = refs[:n_g], refs[n_g:]
    s_refs, (out_ref, g_scr, s_scr, res_scr) = refs[:-4], refs[-4:]
    dp_count, mp_count, parts = sizes["dp_count"], sizes["mp_count"], sizes["parts"]
    piece_rows, tile_cols = sizes["piece_rows"], sizes["tile_cols"]
    slots = mp_count // parts
    order = g_scr.shape[0]
    rows = s_refs[0].shape[1]
    my_index = lax.axis_index("mp")
    slot, part = my_index // parts, my_index % parts
    if split:
        gather_grad(g_refs, g_scr, part, **sizes)
    else:
        g_scr[...] = g_refs[0][...]
    for k in range(parts):
        for j in range(slots):
            chunk = (slot - j + slots) % slots * parts + (part - k + parts) % parts
            s_scr[:, pl.ds(pl.multiple_of(chunk * rows, rows), rows), :] = s_refs[k * slots + j][...]
    ids = lax.broadcasted_iota(jnp.int32, (order, order), 0)
    eye = ids == lax.broadcasted_iota(jnp.int32, (order, order), 1)
    grad = g_scr[...]
    roots = []
    for side in range(2):
        across = 1 - side
        gram = dot(grad, grad, (((across,), (across,)), ((), ())))
        updated = decay_rate * s_scr[side].astype(f32) + (1.0 - decay_rate) * gram
        factor = (updated + jnp.where(eye, damping, 0.0)).astype(bf16)
        roots.append(newton_root(factor, jnp.where(eye, 5.0, 0.0)))
    right_applied = dot(grad, roots[1]).astype(bf16)
    result = dot(roots[0], right_applied).astype(bf16).astype(f32)
    grad_norm = jnp.sqrt(jnp.sum(jnp.square(grad.astype(f32))))
    result_norm = jnp.sqrt(jnp.sum(jnp.square(result)))
    res_scr[...] = (result * (grad_norm / (result_norm + 1e-06))).astype(bf16)
    if split:
        at = pl.multiple_of(part * piece_rows, piece_rows)
        for o in range(dp_count):
            for m in range(mp_count):
                from_rows = pl.ds(o * parts * piece_rows + at, piece_rows)
                out_ref[o * mp_count + m] = res_scr[from_rows, m * tile_cols : (m + 1) * tile_cols]
    else:
        out_ref[...] = res_scr[...]


def stats_kernel(*refs, sizes):
    g_refs, (old_ref, new_ref, g_scr) = refs[:-3], refs[-3:]
    parts = sizes["parts"]
    slots = sizes["mp_count"] // parts
    rows = old_ref.shape[2]
    my_index = lax.axis_index("mp")
    at = pl.multiple_of(my_index * rows, rows)
    for j in range(slots):
        gather_grad(g_refs[j * parts : (j + 1) * parts], g_scr.at[j], my_index % parts, **sizes)
        slot = (my_index // parts - j + slots) % slots
        left = dot(g_scr[j, pl.ds(at, rows), :], g_scr[j], (((1,), (1,)), ((), ())))
        right = dot(g_scr[j, :, pl.ds(at, rows)], g_scr[j], (((0,), (0,)), ((), ())))
        new_ref[slot, 0] = decay_rate * old_ref[slot, 0] + (1.0 - decay_rate) * left
        new_ref[slot, 1] = decay_rate * old_ref[slot, 1] + (1.0 - decay_rate) * right


def call(kernel, out_shape, in_specs, scratch=(), vmem=16, flops=0):
    return pl.pallas_call(
        kernel,
        out_shape=out_shape,
        in_specs=in_specs,
        out_specs=VMEM,
        scratch_shapes=list(scratch),
        compiler_params=pltpu.CompilerParams(vmem_limit_bytes=vmem * 2**20),
        cost_estimate=pl.CostEstimate(flops=flops, transcendentals=0, bytes_accessed=0) if flops else None,
    )


def body(grad_tiles, factor_stats, owner_blocks, rotation):
    dp_count = lax.axis_size("dp")
    mp_count = lax.axis_size("mp")
    tile_rows, tile_cols = grad_tiles.shape[1:]
    slots = owner_blocks.shape[1]
    rows, order = factor_stats.shape[2:]
    parts = mp_count // slots
    piece_rows = tile_rows // parts
    split = piece_rows % 16 == 0 and tile_cols % 128 == 0 and rows == tile_cols
    my_index = lax.axis_index("mp")
    my_slot = my_index // parts
    my_part = my_index % parts
    owners = owner_blocks.T
    where = dict(dp_count=dp_count, slots=slots)
    sizes = dict(
        dp_count=dp_count, mp_count=mp_count, parts=parts, piece_rows=piece_rows, tile_cols=tile_cols
    )

    def to_slot(x, ahead):
        return lax.ppermute(x, "mp", [(i, (i + ahead * parts) % mp_count) for i in range(mp_count)])

    def to_part(x, ahead):
        return lax.ppermute(
            x, "mp", [(i, i // parts * parts + (i + ahead) % parts) for i in range(mp_count)]
        )

    def all_pieces(x):
        return [x] + [to_part(x, ahead) for ahead in range(1, parts)]

    def whole_grad(pieces):
        held = jnp.take(jnp.stack(pieces), (my_part - jnp.arange(parts)) % parts, axis=0)
        held = held.reshape(parts, dp_count, mp_count, piece_rows, tile_cols)
        return held.transpose(1, 0, 3, 2, 4).reshape(order, order)

    chunks = []
    for ahead in range(slots):
        old = lax.dynamic_index_in_dim(factor_stats, (my_slot + ahead) % slots, 0, keepdims=False)
        chunks.append(to_slot(old.astype(bf16), ahead) if ahead else old.astype(bf16))
    chunks += [to_part(chunk, ahead) for ahead in range(1, parts) for chunk in chunks]

    picked = call(
        functools.partial(pick_kernel, **where),
        jax.ShapeDtypeStruct(grad_tiles.shape, bf16),
        [SMEM, SMEM, VMEM],
    )(owners, rotation, grad_tiles)
    outgoing = picked.reshape(dp_count * mp_count, piece_rows, tile_cols)
    arrived = lax.all_to_all(outgoing, ("dp", "mp"), split_axis=0, concat_axis=0, tiled=True)
    pieces = all_pieces(arrived)
    theirs = [to_slot(arrived, ahead) for ahead in range(1, slots)]

    own_grad = pieces if split else [whole_grad(pieces)]
    result = call(
        functools.partial(owner_kernel, n_g=len(own_grad), split=split, sizes=sizes),
        jax.ShapeDtypeStruct(arrived.shape if split else (order, order), bf16),
        [VMEM] * (len(own_grad) + len(chunks)),
        [
            pltpu.VMEM((order, order), bf16),
            pltpu.VMEM((2, order, order), bf16),
            pltpu.VMEM((order, order), bf16),
        ],
        vmem=32,
        flops=24 * order**3,
    )(*own_grad, *chunks)
    if not split:
        result = result.reshape(dp_count, parts, piece_rows, mp_count, tile_cols)
        result = lax.dynamic_index_in_dim(result, my_part, 1, keepdims=False)
        result = result.transpose(0, 2, 1, 3).reshape(dp_count * mp_count, piece_rows, tile_cols)
    returned = lax.all_to_all(result, ("dp", "mp"), split_axis=0, concat_axis=0, tiled=True)

    grads = [pieces] + [all_pieces(x) for x in theirs]
    if split:
        new_stats = call(
            functools.partial(stats_kernel, sizes=sizes),
            jax.ShapeDtypeStruct(factor_stats.shape, f32),
            [VMEM] * (slots * parts + 1),
            [pltpu.VMEM((slots, order, order), bf16)],
            flops=4 * slots * rows * order**2,
        )(*[x for slot_pieces in grads for x in slot_pieces], factor_stats)
    else:
        blocks = jnp.stack([whole_grad(x) for x in grads])
        blocks = jnp.take(blocks, (my_slot - jnp.arange(slots)) % slots, axis=0)
        row_part = lax.dynamic_slice_in_dim(blocks, my_index * rows, rows, 1)
        col_part = lax.dynamic_slice_in_dim(blocks, my_index * rows, rows, 2)
        left = jnp.einsum("kij,klj->kil", row_part, blocks, preferred_element_type=f32)
        right = jnp.einsum("kji,kjl->kil", col_part, blocks, preferred_element_type=f32)
        new_stats = decay_rate * factor_stats + (1.0 - decay_rate) * jnp.stack([left, right], axis=1)

    preconditioned = call(
        functools.partial(place_kernel, **where),
        jax.ShapeDtypeStruct(grad_tiles.shape, bf16),
        [SMEM, SMEM, VMEM],
    )(owners, rotation, returned.reshape(grad_tiles.shape))
    return (preconditioned, new_stats)


def solution(mesh):
    return jax.shard_map(
        body,
        mesh=mesh,
        in_specs=(P(None, "dp", "mp"), P("dp", None, "mp", None), P(), P()),
        out_specs=(P(None, "dp", "mp"), P("dp", None, "mp", None)),
        check_vma=False,
    )
```

```python
import functools

import jax
import jax.numpy as jnp
from jax import lax
from jax.experimental import pallas as pl
from jax.experimental.pallas import tpu as pltpu
from jax.sharding import PartitionSpec as P


ITERS = 2


decay_rate = 0.9
damping = 1.0
bf16 = jnp.bfloat16
f32 = jnp.float32


def owner_of(owners_ref, rot, o, s, dp_count):
    row = o - rot
    return owners_ref[s, jnp.where(row < 0, row + dp_count, row)]


def pick_kernel(owners_hbm, rot_ref, tiles_hbm, out_ref, owners_ref, tiles_ref, sems, *, dp_count, slots):
    pairs = ((owners_hbm, owners_ref), (tiles_hbm, tiles_ref))
    copies = [pltpu.make_async_copy(a, b, sems.at[i]) for i, (a, b) in enumerate(pairs)]
    for copy in copies:
        copy.start()
    for copy in copies:
        copy.wait()
    rot = rot_ref[0]

    def one(j, carry):
        out_ref[j] = tiles_ref[owner_of(owners_ref, rot, j // slots, j % slots, dp_count)]
        return carry

    lax.fori_loop(0, dp_count * slots, one, 0, unroll=dp_count * slots <= 16)


def place_kernel(owners_ref, rot_ref, in_ref, out_hbm, sems, *, dp_count, slots):
    rot = rot_ref[0]

    def copy(j):
        block = owner_of(owners_ref, rot, j // slots, j % slots, dp_count)
        return pltpu.make_async_copy(in_ref.at[j], out_hbm.at[block], sems.at[j])

    def start(j, carry):
        copy(j).start()
        return carry

    def wait(j, carry):
        copy(j).wait()
        return carry

    count = dp_count * slots
    lax.fori_loop(0, count, start, 0, unroll=count <= 16)
    lax.fori_loop(0, count, wait, 0, unroll=count <= 16)


def dot(a, b, dims=(((1,), (0,)), ((), ()))):
    return lax.dot_general(a, b, dims, preferred_element_type=f32)


def newton_root(factor, eye5):
    norm = jnp.sum(jnp.square(factor.astype(f32)))
    moment = (2.5 / jnp.sqrt(norm) * factor.astype(f32)).astype(bf16)
    current = None
    for newton_step in range(ITERS):
        step_t = ((eye5 - moment.astype(f32)) * 0.25).astype(bf16)
        current = step_t if newton_step == 0 else dot(current, step_t).astype(bf16)
        if newton_step + 1 < ITERS:
            square = dot(step_t, step_t).astype(bf16)
            partial_m = dot(square, moment).astype(bf16)
            moment = dot(square, partial_m).astype(bf16)
    return current


def gather_grad(g_refs, g_scr, part, *, dp_count, mp_count, parts, piece_rows, tile_cols):
    for k, g_ref in enumerate(g_refs):
        piece = part - k
        at = pl.multiple_of(jnp.where(piece < 0, piece + parts, piece) * piece_rows, piece_rows)
        for o in range(dp_count):
            for m in range(mp_count):
                rows = pl.ds(o * parts * piece_rows + at, piece_rows)
                g_scr[rows, m * tile_cols : (m + 1) * tile_cols] = g_ref[o * mp_count + m]


def base_kernel(*refs, parts):
    s_refs, (out_ref, s_scr) = refs[:-2], refs[-2:]
    order = out_ref.shape[0]
    rows = s_refs[0].shape[0]
    my_index = lax.axis_index("mp")
    half = rows * parts
    for k, s_ref in enumerate(s_refs):
        at = pl.multiple_of((my_index ^ k) * rows, rows)
        if s_ref.shape[1] == order:
            s_scr[pl.ds(at, rows), :] = s_ref[...]
            continue
        for slot in range(2):

            @pl.when(my_index // parts == slot)
            def _():
                s_scr[pl.ds(at, rows), (1 - slot) * half : (2 - slot) * half] = s_ref[...]

    if s_refs[-1].shape[1] != order:
        for slot in range(2):

            @pl.when(my_index // parts == slot)
            def _():
                mine = slice(slot * half, (slot + 1) * half)
                other = slice((1 - slot) * half, (2 - slot) * half)
                s_scr[other, mine] = s_scr[mine, other].astype(f32).T.astype(bf16)

    ids = lax.broadcasted_iota(jnp.int32, (order, order), 0)
    eye = ids == lax.broadcasted_iota(jnp.int32, (order, order), 1)
    out_ref[...] = decay_rate * s_scr[...].astype(f32) + jnp.where(eye, damping, 0.0)


def root_kernel(*refs, n_g, split, sizes):
    g_refs, (base_ref, root_ref, grad_ref, gram_scr) = refs[:n_g], refs[n_g:]
    order = grad_ref.shape[0]
    part = lax.axis_index("mp") % sizes["parts"]
    if split:
        gather_grad(g_refs, grad_ref, part, **sizes)
    else:
        grad_ref[...] = g_refs[0][...]
    for side in range(2):

        @pl.when(part % 2 == side)
        def _():
            across = 1 - side
            gram_scr[...] = dot(grad_ref[...], grad_ref[...], (((across,), (across,)), ((), ())))

    ids = lax.broadcasted_iota(jnp.int32, (order, order), 0)
    eye = ids == lax.broadcasted_iota(jnp.int32, (order, order), 1)
    factor = (base_ref[...] + (1.0 - decay_rate) * gram_scr[...]).astype(bf16)
    root_ref[...] = newton_root(factor, jnp.where(eye, 5.0, 0.0))


def half_kernel(root_ref, grad_ref, out_ref, norm_ref, *, parts):
    for side in range(2):

        @pl.when(lax.axis_index("mp") % parts % 2 == side)
        def _():
            a, b = (root_ref, grad_ref) if side == 0 else (grad_ref, root_ref)
            out_ref[...] = dot(a[...], b[...]).astype(bf16)

    squares = jnp.sum(jnp.square(grad_ref[...].astype(f32)))
    norm_ref[...] = jnp.full(norm_ref.shape, jnp.sqrt(squares), f32)


def result_kernel(half_ref, root_ref, norm_ref, out_ref, res_scr, *, split, sizes):
    dp_count, mp_count, parts = sizes["dp_count"], sizes["mp_count"], sizes["parts"]
    piece_rows, tile_cols = sizes["piece_rows"], sizes["tile_cols"]
    part = lax.axis_index("mp") % parts
    for side in range(2):

        @pl.when(part % 2 == side)
        def _():
            a, b = (half_ref, root_ref) if side == 0 else (root_ref, half_ref)
            res_scr[...] = dot(a[...], b[...]).astype(bf16)

    scale = norm_ref[0, 0] / (jnp.sqrt(jnp.sum(jnp.square(res_scr[...].astype(f32)))) + 1e-06)
    if not split:
        out_ref[...] = (res_scr[...].astype(f32) * scale).astype(bf16)
        return
    at = pl.multiple_of(part * piece_rows, piece_rows)
    for o in range(dp_count):
        for m in range(mp_count):
            piece = res_scr[pl.ds(o * parts * piece_rows + at, piece_rows), m * tile_cols : (m + 1) * tile_cols]
            out_ref[o * mp_count + m] = (piece.astype(f32) * scale).astype(bf16)


def stats_kernel(*refs, sizes):
    g_refs, (old_ref, new_ref, g_scr) = refs[:-3], refs[-3:]
    parts = sizes["parts"]
    slots = sizes["mp_count"] // parts
    rows = old_ref.shape[2]
    my_index = lax.axis_index("mp")
    at = pl.multiple_of(my_index * rows, rows)
    for j in range(slots):
        gather_grad(g_refs[j * parts : (j + 1) * parts], g_scr.at[j], my_index % parts, **sizes)
        slot = (my_index // parts - j + slots) % slots
        left = dot(g_scr[j, pl.ds(at, rows), :], g_scr[j], (((1,), (1,)), ((), ())))
        right = dot(g_scr[j, :, pl.ds(at, rows)], g_scr[j], (((0,), (0,)), ((), ())))
        new_ref[slot, 0] = decay_rate * old_ref[slot, 0] + (1.0 - decay_rate) * left
        new_ref[slot, 1] = decay_rate * old_ref[slot, 1] + (1.0 - decay_rate) * right


VMEM = pl.BlockSpec(memory_space=pltpu.VMEM)
SMEM = pl.BlockSpec(memory_space=pltpu.SMEM)
HBM = pl.BlockSpec(memory_space=pltpu.HBM)


def in_hbm(x):
    return pltpu.with_memory_space_constraint(x, pltpu.HBM)


def call(kernel, out_shape, in_specs, scratch=(), out_specs=VMEM, vmem=8, flops=0):
    return pl.pallas_call(
        kernel,
        out_shape=out_shape,
        in_specs=in_specs,
        out_specs=(VMEM,) * len(out_shape) if isinstance(out_shape, tuple) else out_specs,
        scratch_shapes=list(scratch),
        compiler_params=pltpu.CompilerParams(vmem_limit_bytes=vmem * 2**20),
        cost_estimate=pl.CostEstimate(flops=flops, transcendentals=0, bytes_accessed=0) if flops else None,
    )


def step(grad_tiles, factor_stats, owner_blocks, rotation):
    dp_count = lax.axis_size("dp")
    mp_count = lax.axis_size("mp")
    tile_rows, tile_cols = grad_tiles.shape[1:]
    slots = owner_blocks.shape[1]
    rows, order = factor_stats.shape[2:]
    parts = mp_count // slots
    assert parts % 2 == 0 and mp_count & (mp_count - 1) == 0
    piece_rows = tile_rows // parts
    split = piece_rows % 16 == 0 and tile_cols % 128 == 0 and rows == tile_cols
    my_index = lax.axis_index("mp")
    my_slot = my_index // parts
    my_part = my_index % parts
    owners = owner_blocks.T
    where = dict(dp_count=dp_count, slots=slots)
    sizes = dict(
        dp_count=dp_count, mp_count=mp_count, parts=parts, piece_rows=piece_rows, tile_cols=tile_cols
    )
    table = pltpu.SMEM(owners.shape, jnp.int32)

    def to_slot(x, ahead):
        return lax.ppermute(x, "mp", [(i, (i + ahead * parts) % mp_count) for i in range(mp_count)])

    def to_part(x, ahead):
        return lax.ppermute(
            x, "mp", [(i, i // parts * parts + (i + ahead) % parts) for i in range(mp_count)]
        )

    def to_flip(x, flip):
        return lax.ppermute(x, "mp", [(i, i ^ flip) for i in range(mp_count)])

    def all_pieces(x):
        return [x] + [to_part(x, ahead) for ahead in range(1, parts)]

    def whole_grad(pieces):
        held = jnp.take(jnp.stack(pieces), (my_part - jnp.arange(parts)) % parts, axis=0)
        held = held.reshape(parts, dp_count, mp_count, piece_rows, tile_cols)
        return held.transpose(1, 0, 3, 2, 4).reshape(order, order)

    square = pltpu.VMEM((order, order), bf16)
    square_f32 = pltpu.VMEM((order, order), f32)
    chunks = []
    for flip in range(mp_count):
        dest = my_index ^ flip
        across = flip >= parts and slots == 2
        at = (dest // parts, dest % parts % 2, 0, my_slot * rows * parts if across else 0)
        old = lax.dynamic_slice(factor_stats, at, (1, 1, rows, rows * parts if across else order))
        old = old.reshape(old.shape[2:]).astype(bf16)
        chunks.append(to_flip(old, flip) if flip else old)
    base = call(
        functools.partial(base_kernel, parts=parts),
        square_f32,
        [VMEM] * len(chunks),
        [square],
        flops=order**2,
    )(*chunks)

    picked = call(
        functools.partial(pick_kernel, **where),
        jax.ShapeDtypeStruct(grad_tiles.shape, bf16),
        [HBM, SMEM, HBM],
        [table, pltpu.VMEM(grad_tiles.shape, bf16), pltpu.SemaphoreType.DMA((2,))],
    )(in_hbm(owners), rotation, in_hbm(grad_tiles))
    outgoing = picked.reshape(dp_count * mp_count, piece_rows, tile_cols)
    arrived = lax.all_to_all(outgoing, ("dp", "mp"), split_axis=0, concat_axis=0, tiled=True)
    pieces = all_pieces(arrived)
    theirs = [to_slot(arrived, ahead) for ahead in range(1, slots)]

    own_grad = pieces if split else [whole_grad(pieces)]
    root, grad = call(
        functools.partial(root_kernel, n_g=len(own_grad), split=split, sizes=sizes),
        (square, square),
        [VMEM] * (len(own_grad) + 1),
        [square_f32],
        vmem=16,
        flops=10 * order**3,
    )(*own_grad, base)
    other_root = to_flip(root, 1)
    half, norm = call(
        functools.partial(half_kernel, parts=parts),
        (square, pltpu.VMEM((8, 128), f32)),
        [VMEM, VMEM],
        flops=2 * order**3,
    )(root, grad)
    result = call(
        functools.partial(result_kernel, split=split, sizes=sizes),
        pltpu.VMEM(arrived.shape if split else (order, order), bf16),
        [VMEM, VMEM, VMEM],
        [square],
        flops=2 * order**3,
    )(half, other_root, norm)
    if not split:
        result = result.reshape(dp_count, parts, piece_rows, mp_count, tile_cols)
        result = lax.dynamic_index_in_dim(result, my_part, 1, keepdims=False)
        result = result.transpose(0, 2, 1, 3).reshape(dp_count * mp_count, piece_rows, tile_cols)
    returned = lax.all_to_all(result, ("dp", "mp"), split_axis=0, concat_axis=0, tiled=True)

    grads = [pieces] + [all_pieces(x) for x in theirs]
    if split:
        new_stats = call(
            functools.partial(stats_kernel, sizes=sizes),
            jax.ShapeDtypeStruct(factor_stats.shape, f32),
            [VMEM] * (slots * parts + 1),
            [pltpu.VMEM((slots, order, order), bf16)],
            vmem=16,
            flops=4 * slots * rows * order**2,
        )(*[x for slot_pieces in grads for x in slot_pieces], factor_stats)
    else:
        blocks = jnp.stack([whole_grad(x) for x in grads])
        blocks = jnp.take(blocks, (my_slot - jnp.arange(slots)) % slots, axis=0)
        row_part = lax.dynamic_slice_in_dim(blocks, my_index * rows, rows, 1)
        col_part = lax.dynamic_slice_in_dim(blocks, my_index * rows, rows, 2)
        left = jnp.einsum("kij,klj->kil", row_part, blocks, preferred_element_type=f32)
        right = jnp.einsum("kji,kjl->kil", col_part, blocks, preferred_element_type=f32)
        new_stats = decay_rate * factor_stats + (1.0 - decay_rate) * jnp.stack([left, right], axis=1)

    preconditioned = call(
        functools.partial(place_kernel, **where),
        jax.ShapeDtypeStruct(grad_tiles.shape, bf16),
        [SMEM, SMEM, VMEM],
        [pltpu.SemaphoreType.DMA((dp_count * slots,))],
        out_specs=HBM,
    )(owners, rotation, returned.reshape(grad_tiles.shape))
    return (preconditioned, new_stats)


def solution(mesh):
    return placed(mesh)


def placed(mesh):
    return jax.shard_map(
        step,
        mesh=mesh,
        in_specs=(P(None, "dp", "mp"), P("dp", None, "mp", None), P(), P()),
        out_specs=(P(None, "dp", "mp"), P("dp", None, "mp", None)),
        check_vma=False,
    )
```

```python
import functools

import jax
import jax.numpy as jnp
from jax import lax
from jax.experimental import pallas as pl
from jax.experimental.pallas import tpu as pltpu
from jax.sharding import PartitionSpec as P


ITERS = 2


decay_rate = 0.9
damping = 1.0
bf16 = jnp.bfloat16
f32 = jnp.float32


def owner_of(owners_ref, rot, o, s, dp_count):
    row = o - rot
    return owners_ref[s, jnp.where(row < 0, row + dp_count, row)]


def each(count, one):
    lax.fori_loop(0, count, lambda j, carry: (one(j), carry)[1], 0, unroll=count <= 16)


def pick_kernel(
    owners_hbm, rot_ref, tiles_hbm, stats_hbm, out_ref, far_ref, near_ref, owners_ref, tiles_ref, far_scr, near_scr, sems,
    *, dp_count, parts
):
    slots = owners_ref.shape[0]
    half = far_scr.shape[2]
    slot = lax.axis_index("mp") // parts
    columns = pl.ds(pl.multiple_of(slot * half, half), half)
    pairs = (
        (owners_hbm, owners_ref),
        (tiles_hbm, tiles_ref),
        (stats_hbm.at[1 - slot, :, :, columns], far_scr),
        (stats_hbm.at[slot], near_scr),
    )
    copies = [pltpu.make_async_copy(a, b, sems.at[i]) for i, (a, b) in enumerate(pairs)]
    for copy in copies:
        copy.start()
    rot = rot_ref[0]
    copies[0].wait()
    copies[1].wait()

    def move(j):
        out_ref[j] = tiles_ref[owner_of(owners_ref, rot, j // slots, j % slots, dp_count)]

    each(dp_count * slots, move)
    copies[2].wait()
    far_ref[...] = far_scr[...].astype(bf16)
    copies[3].wait()
    near_ref[...] = near_scr[...].astype(bf16)


def place_kernel(owners_ref, rot_ref, in_ref, out_hbm, sems, *, dp_count, slots):
    rot = rot_ref[0]

    def copy(j):
        block = owner_of(owners_ref, rot, j // slots, j % slots, dp_count)
        return pltpu.make_async_copy(in_ref.at[j], out_hbm.at[block], sems.at[j])

    each(dp_count * slots, lambda j: copy(j).start())
    each(dp_count * slots, lambda j: copy(j).wait())


def dot(a, b, dims=(((1,), (0,)), ((), ()))):
    return lax.dot_general(a, b, dims, preferred_element_type=f32)


def gather_grad(g_refs, g_scr, part, *, dp_count, mp_count, parts, piece_rows, tile_cols):
    for k, g_ref in enumerate(g_refs):
        piece = part - k
        at = pl.multiple_of(jnp.where(piece < 0, piece + parts, piece) * piece_rows, piece_rows)
        for o in range(dp_count):
            for m in range(mp_count):
                rows = pl.ds(o * parts * piece_rows + at, piece_rows)
                g_scr[rows, m * tile_cols : (m + 1) * tile_cols] = g_ref[o * mp_count + m]


def base_kernel(*refs, parts, slots):
    s_refs, (out_ref, s_scr) = refs[:-2], refs[-2:]
    order = out_ref.shape[1]
    rows = s_refs[0].shape[1]
    half = rows * parts
    my_index = lax.axis_index("mp")
    slot, part = my_index // parts, my_index % parts
    for i, s_ref in enumerate(s_refs):
        k, j = i // slots, i % slots
        source = (slot - j + slots) % slots * parts + (part - k + parts) % parts
        at = pl.multiple_of(source * rows, rows)
        if s_ref.shape[2] == order:
            s_scr[:, pl.ds(at, rows), :] = s_ref[...]
            continue
        for g in range(2):

            @pl.when(slot == g)
            def _():
                s_scr[:, pl.ds(at, rows), (1 - g) * half : (2 - g) * half] = s_ref[...]

    if slots == 2:
        for g in range(2):

            @pl.when(slot == g)
            def _():
                mine = slice(g * half, (g + 1) * half)
                other = slice((1 - g) * half, (2 - g) * half)
                for side in range(2):
                    s_scr[side, other, mine] = s_scr[side, mine, other].astype(f32).T.astype(bf16)

    ids = lax.broadcasted_iota(jnp.int32, (order, order), 0)
    eye = ids == lax.broadcasted_iota(jnp.int32, (order, order), 1)
    for side in range(2):
        out_ref[side] = decay_rate * s_scr[side].astype(f32) + jnp.where(eye, damping, 0.0)


def owner_kernel(*refs, n_g, split, sizes):
    g_refs, (base_ref, out_ref, g_scr, res_scr) = refs[:n_g], refs[n_g:]
    dp_count, mp_count, parts = sizes["dp_count"], sizes["mp_count"], sizes["parts"]
    piece_rows, tile_cols = sizes["piece_rows"], sizes["tile_cols"]
    order = g_scr.shape[0]
    part = lax.axis_index("mp") % parts
    if split:
        gather_grad(g_refs, g_scr, part, **sizes)
    else:
        g_scr[...] = g_refs[0][...]
    ids = lax.broadcasted_iota(jnp.int32, (order, order), 0)
    eye5 = jnp.where(ids == lax.broadcasted_iota(jnp.int32, (order, order), 1), 5.0, 0.0)
    grad = g_scr[...]

    def gram_of(side):
        return dot(grad, grad, (((1 - side,), (1 - side,)), ((), ())))

    def moment_of(side, gram):
        factor = (base_ref[side] + (1.0 - decay_rate) * gram).astype(bf16)
        norm = jnp.sum(jnp.square(factor.astype(f32)))
        return (2.5 / jnp.sqrt(norm) * factor.astype(f32)).astype(bf16)

    def step_of(moment):
        return ((eye5 - moment.astype(f32)) * 0.25).astype(bf16)

    def product(a, b):
        return dot(a, b).astype(bf16)

    grams = {1: gram_of(1), 0: gram_of(0)}
    moment = {1: moment_of(1, grams[1])}
    root = {1: step_of(moment[1])}
    for newton_step in range(ITERS - 1):
        step_t = {1: root[1] if newton_step == 0 else step_of(moment[1])}
        square = {1: product(step_t[1], step_t[1])}
        if newton_step == 0:
            moment[0] = moment_of(0, grams[0])
            root[0] = step_of(moment[0])
        else:
            root[1] = product(root[1], step_t[1])
        step_t[0] = root[0] if newton_step == 0 else step_of(moment[0])
        partial_m = {1: product(square[1], moment[1])}
        square[0] = product(step_t[0], step_t[0])
        if newton_step:
            root[0] = product(root[0], step_t[0])
        moment[1] = product(square[1], partial_m[1])
        partial_m[0] = product(square[0], moment[0])
        last = step_of(moment[1])
        moment[0] = product(square[0], partial_m[0])
    root[1] = product(root[1], last)
    last = step_of(moment[0])
    right_applied = product(grad, root[1])
    root[0] = product(root[0], last)
    res_scr[...] = dot(root[0], right_applied).astype(bf16)
    grad_norm = jnp.sqrt(jnp.sum(jnp.square(grad.astype(f32))))
    scale = grad_norm / (jnp.sqrt(jnp.sum(jnp.square(res_scr[...].astype(f32)))) + 1e-06)
    if not split:
        out_ref[...] = (res_scr[...].astype(f32) * scale).astype(bf16)
        return
    at = pl.multiple_of(part * piece_rows, piece_rows)
    for o in range(dp_count):
        for m in range(mp_count):
            from_rows = pl.ds(o * parts * piece_rows + at, piece_rows)
            piece = res_scr[from_rows, m * tile_cols : (m + 1) * tile_cols].astype(f32)
            out_ref[o * mp_count + m] = (piece * scale).astype(bf16)


def stats_kernel(*refs, sizes):
    g_refs, (old_hbm, new_ref, g_scr, old_ref, sem) = refs[:-5], refs[-5:]
    parts = sizes["parts"]
    slots = sizes["mp_count"] // parts
    rows = old_ref.shape[2]
    old = pltpu.make_async_copy(old_hbm, old_ref, sem)
    old.start()
    my_index = lax.axis_index("mp")
    at = pl.multiple_of(my_index * rows, rows)
    for j in range(slots):
        gather_grad(g_refs[j * parts : (j + 1) * parts], g_scr.at[j], my_index % parts, **sizes)
        slot = (my_index // parts - j + slots) % slots
        left = dot(g_scr[j, pl.ds(at, rows), :], g_scr[j], (((1,), (1,)), ((), ())))
        right = dot(g_scr[j, :, pl.ds(at, rows)], g_scr[j], (((0,), (0,)), ((), ())))
        if j == 0:
            old.wait()
        new_ref[slot, 0] = decay_rate * old_ref[slot, 0] + (1.0 - decay_rate) * left
        new_ref[slot, 1] = decay_rate * old_ref[slot, 1] + (1.0 - decay_rate) * right


VMEM = pl.BlockSpec(memory_space=pltpu.VMEM)
SMEM = pl.BlockSpec(memory_space=pltpu.SMEM)
HBM = pl.BlockSpec(memory_space=pltpu.HBM)


def in_hbm(x):
    return pltpu.with_memory_space_constraint(x, pltpu.HBM)


def call(kernel, out_shape, in_specs, scratch=(), out_specs=VMEM, vmem=8, flops=0):
    return pl.pallas_call(
        kernel,
        out_shape=out_shape,
        in_specs=in_specs,
        out_specs=out_specs,
        scratch_shapes=list(scratch),
        compiler_params=pltpu.CompilerParams(vmem_limit_bytes=vmem * 2**20),
        cost_estimate=pl.CostEstimate(flops=flops, transcendentals=0, bytes_accessed=0) if flops else None,
    )


def step(grad_tiles, factor_stats, owner_blocks, rotation):
    dp_count = lax.axis_size("dp")
    mp_count = lax.axis_size("mp")
    tile_rows, tile_cols = grad_tiles.shape[1:]
    slots = owner_blocks.shape[1]
    rows, order = factor_stats.shape[2:]
    parts = mp_count // slots
    piece_rows = tile_rows // parts
    split = piece_rows % 16 == 0 and tile_cols % 128 == 0 and rows == tile_cols
    my_index = lax.axis_index("mp")
    my_slot = my_index // parts
    my_part = my_index % parts
    owners = owner_blocks.T
    where = dict(dp_count=dp_count, slots=slots)
    sizes = dict(
        dp_count=dp_count, mp_count=mp_count, parts=parts, piece_rows=piece_rows, tile_cols=tile_cols
    )
    table = pltpu.SMEM(owners.shape, jnp.int32)

    def to_slot(x, ahead):
        return lax.ppermute(x, "mp", [(i, (i + ahead * parts) % mp_count) for i in range(mp_count)])

    def to_part(x, ahead):
        return lax.ppermute(
            x, "mp", [(i, i // parts * parts + (i + ahead) % parts) for i in range(mp_count)]
        )

    def all_pieces(x):
        return [x] + [to_part(x, ahead) for ahead in range(1, parts)]

    def whole_grad(pieces):
        held = jnp.take(jnp.stack(pieces), (my_part - jnp.arange(parts)) % parts, axis=0)
        held = held.reshape(parts, dp_count, mp_count, piece_rows, tile_cols)
        return held.transpose(1, 0, 3, 2, 4).reshape(order, order)

    assert slots == 2
    half = rows * parts
    picked, far, near, table = call(
        functools.partial(pick_kernel, dp_count=dp_count, parts=parts),
        (
            pltpu.VMEM(grad_tiles.shape, bf16),
            pltpu.VMEM((2, rows, half), bf16),
            pltpu.VMEM((2, rows, order), bf16),
            pltpu.SMEM(owners.shape, jnp.int32),
        ),
        [HBM, SMEM, HBM, HBM],
        [
            pltpu.VMEM(grad_tiles.shape, bf16),
            pltpu.VMEM((2, rows, half), f32),
            pltpu.VMEM((2, rows, order), f32),
            pltpu.SemaphoreType.DMA((4,)),
        ],
        out_specs=(VMEM, VMEM, VMEM, SMEM),
    )(in_hbm(owners), rotation, in_hbm(grad_tiles), in_hbm(factor_stats))
    chunks = [near, to_slot(far, 1)]
    for ahead in range(1, parts):
        chunks.append(to_part(near, ahead))
        chunks.append(to_part(chunks[1], ahead))
    base = call(
        functools.partial(base_kernel, parts=parts, slots=slots),
        pltpu.VMEM((2, order, order), f32),
        [VMEM] * len(chunks),
        [pltpu.VMEM((2, order, order), bf16)],
        flops=order**2,
    )(*chunks)

    outgoing = picked.reshape(dp_count * mp_count, piece_rows, tile_cols)
    arrived = lax.all_to_all(outgoing, ("dp", "mp"), split_axis=0, concat_axis=0, tiled=True)
    pieces = all_pieces(arrived)
    theirs = [to_slot(arrived, ahead) for ahead in range(1, slots)]

    own_grad = pieces if split else [whole_grad(pieces)]
    result = call(
        functools.partial(owner_kernel, n_g=len(own_grad), split=split, sizes=sizes),
        pltpu.HBM(arrived.shape if split else (order, order), bf16),
        [VMEM] * (len(own_grad) + 1),
        [pltpu.VMEM((order, order), bf16), pltpu.VMEM((order, order), bf16)],
        vmem=24,
        flops=24 * order**3,
    )(*own_grad, base)
    if not split:
        result = result.reshape(dp_count, parts, piece_rows, mp_count, tile_cols)
        result = lax.dynamic_index_in_dim(result, my_part, 1, keepdims=False)
        result = result.transpose(0, 2, 1, 3).reshape(dp_count * mp_count, piece_rows, tile_cols)
    returned = lax.all_to_all(result, ("dp", "mp"), split_axis=0, concat_axis=0, tiled=True)

    grads = [pieces] + [all_pieces(x) for x in theirs]
    if split:
        new_stats = call(
            functools.partial(stats_kernel, sizes=sizes),
            jax.ShapeDtypeStruct(factor_stats.shape, f32),
            [VMEM] * (slots * parts) + [HBM],
            [
                pltpu.VMEM((slots, order, order), bf16),
                pltpu.VMEM(factor_stats.shape, f32),
                pltpu.SemaphoreType.DMA,
            ],
            vmem=16,
            flops=4 * slots * rows * order**2,
        )(*[x for slot_pieces in grads for x in slot_pieces], in_hbm(factor_stats))
    else:
        blocks = jnp.stack([whole_grad(x) for x in grads])
        blocks = jnp.take(blocks, (my_slot - jnp.arange(slots)) % slots, axis=0)
        row_part = lax.dynamic_slice_in_dim(blocks, my_index * rows, rows, 1)
        col_part = lax.dynamic_slice_in_dim(blocks, my_index * rows, rows, 2)
        left = jnp.einsum("kij,klj->kil", row_part, blocks, preferred_element_type=f32)
        right = jnp.einsum("kji,kjl->kil", col_part, blocks, preferred_element_type=f32)
        new_stats = decay_rate * factor_stats + (1.0 - decay_rate) * jnp.stack([left, right], axis=1)

    preconditioned = call(
        functools.partial(place_kernel, **where),
        jax.ShapeDtypeStruct(grad_tiles.shape, bf16),
        [SMEM, SMEM, VMEM],
        [pltpu.SemaphoreType.DMA((dp_count * slots,))],
        out_specs=HBM,
    )(table, rotation, returned.reshape(grad_tiles.shape))
    return (preconditioned, new_stats)


def solution(mesh):
    return placed(mesh)


def placed(mesh):
    return jax.shard_map(
        step,
        mesh=mesh,
        in_specs=(P(None, "dp", "mp"), P("dp", None, "mp", None), P(), P()),
        out_specs=(P(None, "dp", "mp"), P("dp", None, "mp", None)),
        check_vma=False,
    )
```

```python
import functools

import jax
import jax.numpy as jnp
from jax import lax
from jax.experimental import pallas as pl
from jax.experimental.pallas import tpu as pltpu
from jax.sharding import PartitionSpec as P


ITERS = 2


decay_rate = 0.9
damping = 1.0
bf16 = jnp.bfloat16
f32 = jnp.float32


def owner_of(owners_ref, rot, o, s, dp_count):
    row = o - rot
    return owners_ref[s, jnp.where(row < 0, row + dp_count, row)]


def each(count, one):
    lax.fori_loop(0, count, lambda j, carry: (one(j), carry)[1], 0, unroll=count <= 16)


def pick_kernel(
    owners_hbm, rot_ref, tiles_hbm, stats_hbm, out_ref, far_ref, near_ref, owners_ref, tiles_ref, far_scr, near_scr, sems,
    *, dp_count, parts
):
    slots = owners_ref.shape[0]
    half = far_scr.shape[2]
    slot = lax.axis_index("mp") // parts
    columns = pl.ds(pl.multiple_of(slot * half, half), half)
    pairs = (
        (owners_hbm, owners_ref),
        (tiles_hbm, tiles_ref),
        (stats_hbm.at[1 - slot, :, :, columns], far_scr),
        (stats_hbm.at[slot], near_scr),
    )
    copies = [pltpu.make_async_copy(a, b, sems.at[i]) for i, (a, b) in enumerate(pairs)]
    for copy in copies:
        copy.start()
    rot = rot_ref[0]
    copies[0].wait()
    copies[1].wait()

    def move(j):
        out_ref[j] = tiles_ref[owner_of(owners_ref, rot, j // slots, j % slots, dp_count)]

    each(dp_count * slots, move)
    copies[2].wait()
    far_ref[...] = far_scr[...].astype(bf16)
    copies[3].wait()
    near_ref[...] = near_scr[...].astype(bf16)


def place_kernel(owners_ref, rot_ref, in_ref, out_hbm, sems, *, dp_count, slots):
    rot = rot_ref[0]

    def copy(j):
        block = owner_of(owners_ref, rot, j // slots, j % slots, dp_count)
        return pltpu.make_async_copy(in_ref.at[j], out_hbm.at[block], sems.at[j])

    each(dp_count * slots, lambda j: copy(j).start())
    each(dp_count * slots, lambda j: copy(j).wait())


def dot(a, b, dims=(((1,), (0,)), ((), ()))):
    return lax.dot_general(a, b, dims, preferred_element_type=f32)


def gather_grad(g_refs, g_scr, part, *, dp_count, mp_count, parts, piece_rows, tile_cols):
    for k, g_ref in enumerate(g_refs):
        piece = part - k
        at = pl.multiple_of(jnp.where(piece < 0, piece + parts, piece) * piece_rows, piece_rows)
        for o in range(dp_count):
            for m in range(mp_count):
                rows = pl.ds(o * parts * piece_rows + at, piece_rows)
                g_scr[rows, m * tile_cols : (m + 1) * tile_cols] = g_ref[o * mp_count + m]


def diagonal(shape, value):
    ids = lax.broadcasted_iota(jnp.int32, shape, 0)
    return jnp.where(ids == lax.broadcasted_iota(jnp.int32, shape, 1), value, 0.0)


def near_base_kernel(*refs, parts):
    s_refs, (out_ref, s_scr) = refs[:-2], refs[-2:]
    rows = s_refs[0].shape[1]
    half = rows * parts
    slot, part = lax.axis_index("mp") // parts, lax.axis_index("mp") % parts
    for k, s_ref in enumerate(s_refs):
        at = pl.multiple_of((part - k + parts) % parts * rows, rows)
        s_scr[:, pl.ds(at, rows), :] = s_ref[...]
    for g in range(2):

        @pl.when(slot == g)
        def _():
            mine = slice(g * half, (g + 1) * half)
            other = slice((1 - g) * half, (2 - g) * half)
            for side in range(2):
                square = decay_rate * s_scr[side, :, mine].astype(f32)
                out_ref[side, mine, mine] = square + diagonal((half, half), damping)
                across = decay_rate * s_scr[side, :, other].astype(f32)
                out_ref[side, mine, other] = across
                out_ref[side, other, mine] = across.T


def far_base_kernel(base_ref, *refs, parts):
    s_refs, (out_ref, s_scr) = refs[:-2], refs[-2:]
    rows, half = s_refs[0].shape[1:]
    slot, part = lax.axis_index("mp") // parts, lax.axis_index("mp") % parts
    for k, s_ref in enumerate(s_refs):
        at = pl.multiple_of((part - k + parts) % parts * rows, rows)
        s_scr[:, pl.ds(at, rows), :] = s_ref[...]
    for g in range(2):

        @pl.when(slot == g)
        def _():
            other = slice((1 - g) * half, (2 - g) * half)
            for side in range(2):
                square = decay_rate * s_scr[side].astype(f32)
                out_ref[side, other, other] = square + diagonal((half, half), damping)


def owner_kernel(*refs, n_g, split, sizes):
    g_refs, (base_ref, out_ref, g_scr, res_scr) = refs[:n_g], refs[n_g:]
    dp_count, mp_count, parts = sizes["dp_count"], sizes["mp_count"], sizes["parts"]
    piece_rows, tile_cols = sizes["piece_rows"], sizes["tile_cols"]
    order = g_scr.shape[0]
    part = lax.axis_index("mp") % parts
    if split:
        gather_grad(g_refs, g_scr, part, **sizes)
    else:
        g_scr[...] = g_refs[0][...]
    eye5 = diagonal((order, order), 5.0)
    grad = g_scr[...]

    def gram_of(side):
        return dot(grad, grad, (((1 - side,), (1 - side,)), ((), ())))

    def moment_of(side, gram):
        factor = (base_ref[side] + (1.0 - decay_rate) * gram).astype(bf16)
        norm = jnp.sum(jnp.square(factor.astype(f32)))
        return (2.5 / jnp.sqrt(norm) * factor.astype(f32)).astype(bf16)

    def step_of(moment):
        return ((eye5 - moment.astype(f32)) * 0.25).astype(bf16)

    def product(a, b):
        return dot(a, b).astype(bf16)

    grams = {1: gram_of(1), 0: gram_of(0)}
    moment = {1: moment_of(1, grams[1])}
    root = {1: step_of(moment[1])}
    for newton_step in range(ITERS - 1):
        step_t = {1: root[1] if newton_step == 0 else step_of(moment[1])}
        square = {1: product(step_t[1], step_t[1])}
        if newton_step == 0:
            moment[0] = moment_of(0, grams[0])
            root[0] = step_of(moment[0])
        else:
            root[1] = product(root[1], step_t[1])
        step_t[0] = root[0] if newton_step == 0 else step_of(moment[0])
        partial_m = {1: product(square[1], moment[1])}
        square[0] = product(step_t[0], step_t[0])
        if newton_step:
            root[0] = product(root[0], step_t[0])
        moment[1] = product(square[1], partial_m[1])
        partial_m[0] = product(square[0], moment[0])
        last = step_of(moment[1])
        moment[0] = product(square[0], partial_m[0])
    root[1] = product(root[1], last)
    grad_norm = jnp.sqrt(jnp.sum(jnp.square(grad.astype(f32))))
    last = step_of(moment[0])
    right_applied = product(grad, root[1])
    root[0] = product(root[0], last)
    res_scr[...] = dot(root[0], right_applied).astype(bf16)
    scale = grad_norm / (jnp.sqrt(jnp.sum(jnp.square(res_scr[...].astype(f32)))) + 1e-06)
    if not split:
        out_ref[...] = (res_scr[...].astype(f32) * scale).astype(bf16)
        return
    at = pl.multiple_of(part * piece_rows, piece_rows)
    for o in range(dp_count):
        for m in range(mp_count):
            from_rows = pl.ds(o * parts * piece_rows + at, piece_rows)
            piece = res_scr[from_rows, m * tile_cols : (m + 1) * tile_cols].astype(f32)
            out_ref[o * mp_count + m] = (piece * scale).astype(bf16)


def stats_kernel(*refs, sizes):
    g_refs, (old_hbm, new_ref, g_scr, old_ref, sem) = refs[:-5], refs[-5:]
    parts = sizes["parts"]
    slots = sizes["mp_count"] // parts
    rows = old_ref.shape[2]
    old = pltpu.make_async_copy(old_hbm, old_ref, sem)
    old.start()
    my_index = lax.axis_index("mp")
    at = pl.multiple_of(my_index * rows, rows)
    for j in range(slots):
        gather_grad(g_refs[j * parts : (j + 1) * parts], g_scr.at[j], my_index % parts, **sizes)
        slot = (my_index // parts - j + slots) % slots
        left = dot(g_scr[j, pl.ds(at, rows), :], g_scr[j], (((1,), (1,)), ((), ())))
        right = dot(g_scr[j, :, pl.ds(at, rows)], g_scr[j], (((0,), (0,)), ((), ())))
        if j == 0:
            old.wait()
        new_ref[slot, 0] = decay_rate * old_ref[slot, 0] + (1.0 - decay_rate) * left
        new_ref[slot, 1] = decay_rate * old_ref[slot, 1] + (1.0 - decay_rate) * right


VMEM = pl.BlockSpec(memory_space=pltpu.VMEM)
SMEM = pl.BlockSpec(memory_space=pltpu.SMEM)
HBM = pl.BlockSpec(memory_space=pltpu.HBM)


def in_hbm(x):
    return pltpu.with_memory_space_constraint(x, pltpu.HBM)


def call(kernel, out_shape, in_specs, scratch=(), out_specs=VMEM, vmem=8, flops=0, aliases=None):
    return pl.pallas_call(
        kernel,
        out_shape=out_shape,
        in_specs=in_specs,
        out_specs=out_specs,
        scratch_shapes=list(scratch),
        input_output_aliases=aliases or {},
        compiler_params=pltpu.CompilerParams(vmem_limit_bytes=vmem * 2**20),
        cost_estimate=pl.CostEstimate(flops=flops, transcendentals=0, bytes_accessed=0) if flops else None,
    )


def step(grad_tiles, factor_stats, owner_blocks, rotation):
    dp_count = lax.axis_size("dp")
    mp_count = lax.axis_size("mp")
    tile_rows, tile_cols = grad_tiles.shape[1:]
    slots = owner_blocks.shape[1]
    rows, order = factor_stats.shape[2:]
    parts = mp_count // slots
    piece_rows = tile_rows // parts
    split = piece_rows % 16 == 0 and tile_cols % 128 == 0 and rows == tile_cols
    my_index = lax.axis_index("mp")
    my_slot = my_index // parts
    my_part = my_index % parts
    owners = owner_blocks.T
    where = dict(dp_count=dp_count, slots=slots)
    sizes = dict(
        dp_count=dp_count, mp_count=mp_count, parts=parts, piece_rows=piece_rows, tile_cols=tile_cols
    )
    table = pltpu.SMEM(owners.shape, jnp.int32)

    def to_slot(x, ahead):
        return lax.ppermute(x, "mp", [(i, (i + ahead * parts) % mp_count) for i in range(mp_count)])

    def to_part(x, ahead):
        return lax.ppermute(
            x, "mp", [(i, i // parts * parts + (i + ahead) % parts) for i in range(mp_count)]
        )

    def all_pieces(x):
        return [x] + [to_part(x, ahead) for ahead in range(1, parts)]

    def whole_grad(pieces):
        held = jnp.take(jnp.stack(pieces), (my_part - jnp.arange(parts)) % parts, axis=0)
        held = held.reshape(parts, dp_count, mp_count, piece_rows, tile_cols)
        return held.transpose(1, 0, 3, 2, 4).reshape(order, order)

    assert slots == 2
    half = rows * parts
    picked, far, near, table = call(
        functools.partial(pick_kernel, dp_count=dp_count, parts=parts),
        (
            pltpu.VMEM(grad_tiles.shape, bf16),
            pltpu.VMEM((2, rows, half), bf16),
            pltpu.VMEM((2, rows, order), bf16),
            pltpu.SMEM(owners.shape, jnp.int32),
        ),
        [HBM, SMEM, HBM, HBM],
        [
            pltpu.VMEM(grad_tiles.shape, bf16),
            pltpu.VMEM((2, rows, half), f32),
            pltpu.VMEM((2, rows, order), f32),
            pltpu.SemaphoreType.DMA((4,)),
        ],
        out_specs=(VMEM, VMEM, VMEM, SMEM),
    )(in_hbm(owners), rotation, in_hbm(grad_tiles), in_hbm(factor_stats))
    chunks = [near, to_slot(far, 1)]
    for ahead in range(1, parts):
        chunks.append(to_part(near, ahead))
        chunks.append(to_part(chunks[1], ahead))
    base_type = pltpu.VMEM((2, order, order), f32)
    base = call(
        functools.partial(near_base_kernel, parts=parts),
        base_type,
        [VMEM] * parts,
        [pltpu.VMEM((2, half, order), bf16)],
        flops=order**2,
    )(*chunks[0::2])
    base = call(
        functools.partial(far_base_kernel, parts=parts),
        base_type,
        [VMEM] * (parts + 1),
        [pltpu.VMEM((2, half, half), bf16)],
        flops=order**2,
        aliases={0: 0},
    )(base, *chunks[1::2])

    outgoing = picked.reshape(dp_count * mp_count, piece_rows, tile_cols)
    arrived = lax.all_to_all(outgoing, ("dp", "mp"), split_axis=0, concat_axis=0, tiled=True)
    pieces = all_pieces(arrived)
    theirs = [to_slot(arrived, ahead) for ahead in range(1, slots)]

    own_grad = pieces if split else [whole_grad(pieces)]
    result = call(
        functools.partial(owner_kernel, n_g=len(own_grad), split=split, sizes=sizes),
        pltpu.HBM(arrived.shape if split else (order, order), bf16),
        [VMEM] * (len(own_grad) + 1),
        [pltpu.VMEM((order, order), bf16), pltpu.VMEM((order, order), bf16)],
        vmem=24,
        flops=24 * order**3,
    )(*own_grad, base)
    if not split:
        result = result.reshape(dp_count, parts, piece_rows, mp_count, tile_cols)
        result = lax.dynamic_index_in_dim(result, my_part, 1, keepdims=False)
        result = result.transpose(0, 2, 1, 3).reshape(dp_count * mp_count, piece_rows, tile_cols)
    returned = lax.all_to_all(result, ("dp", "mp"), split_axis=0, concat_axis=0, tiled=True)

    grads = [pieces] + [all_pieces(x) for x in theirs]
    if split:
        new_stats = call(
            functools.partial(stats_kernel, sizes=sizes),
            jax.ShapeDtypeStruct(factor_stats.shape, f32),
            [VMEM] * (slots * parts) + [HBM],
            [
                pltpu.VMEM((slots, order, order), bf16),
                pltpu.VMEM(factor_stats.shape, f32),
                pltpu.SemaphoreType.DMA,
            ],
            vmem=16,
            flops=4 * slots * rows * order**2,
        )(*[x for slot_pieces in grads for x in slot_pieces], in_hbm(factor_stats))
    else:
        blocks = jnp.stack([whole_grad(x) for x in grads])
        blocks = jnp.take(blocks, (my_slot - jnp.arange(slots)) % slots, axis=0)
        row_part = lax.dynamic_slice_in_dim(blocks, my_index * rows, rows, 1)
        col_part = lax.dynamic_slice_in_dim(blocks, my_index * rows, rows, 2)
        left = jnp.einsum("kij,klj->kil", row_part, blocks, preferred_element_type=f32)
        right = jnp.einsum("kji,kjl->kil", col_part, blocks, preferred_element_type=f32)
        new_stats = decay_rate * factor_stats + (1.0 - decay_rate) * jnp.stack([left, right], axis=1)

    preconditioned = call(
        functools.partial(place_kernel, **where),
        jax.ShapeDtypeStruct(grad_tiles.shape, bf16),
        [SMEM, SMEM, VMEM],
        [pltpu.SemaphoreType.DMA((dp_count * slots,))],
        out_specs=HBM,
    )(table, rotation, returned.reshape(grad_tiles.shape))
    return (preconditioned, new_stats)


def solution(mesh):
    return placed(mesh)


def placed(mesh):
    return jax.shard_map(
        step,
        mesh=mesh,
        in_specs=(P(None, "dp", "mp"), P("dp", None, "mp", None), P(), P()),
        out_specs=(P(None, "dp", "mp"), P("dp", None, "mp", None)),
        check_vma=False,
    )
```

```python
import functools

import jax
import jax.numpy as jnp
from jax import lax
from jax.experimental import pallas as pl
from jax.experimental.pallas import tpu as pltpu
from jax.sharding import PartitionSpec as P


decay_rate = 0.9
damping = 1.0
bf16 = jnp.bfloat16
f32 = jnp.float32


def owner_of(owners_ref, rot, o, s, dp_count):
    row = o - rot
    return owners_ref[s, jnp.where(row < 0, row + dp_count, row)]


def each(count, one):
    lax.fori_loop(0, count, lambda j, carry: (one(j), carry)[1], 0, unroll=count <= 16)


def pick_kernel(
    owners_hbm, rot_ref, tiles_hbm, stats_hbm, out_ref, far_ref, near_ref, owners_ref, tiles_ref, far_scr, near_scr, sems,
    *, dp_count, parts
):
    slots = owners_ref.shape[0]
    half = far_scr.shape[2]
    slot = lax.axis_index("mp") // parts
    columns = pl.ds(pl.multiple_of(slot * half, half), half)
    pairs = (
        (owners_hbm, owners_ref),
        (tiles_hbm, tiles_ref),
        (stats_hbm.at[1 - slot, :, :, columns], far_scr),
        (stats_hbm.at[slot], near_scr),
    )
    copies = [pltpu.make_async_copy(a, b, sems.at[i]) for i, (a, b) in enumerate(pairs)]
    for copy in copies:
        copy.start()
    rot = rot_ref[0]
    copies[0].wait()
    copies[1].wait()

    def move(j):
        out_ref[j] = tiles_ref[owner_of(owners_ref, rot, j // slots, j % slots, dp_count)]

    each(dp_count * slots, move)
    copies[2].wait()
    far_ref[...] = far_scr[...].astype(bf16)
    copies[3].wait()
    near_ref[...] = near_scr[...].astype(bf16)


def place_kernel(owners_ref, rot_ref, in_ref, out_hbm, sems, *, dp_count, slots):
    rot = rot_ref[0]

    def copy(j):
        block = owner_of(owners_ref, rot, j // slots, j % slots, dp_count)
        return pltpu.make_async_copy(in_ref.at[j], out_hbm.at[block], sems.at[j])

    each(dp_count * slots, lambda j: copy(j).start())
    each(dp_count * slots, lambda j: copy(j).wait())


def dot(a, b, dims=(((1,), (0,)), ((), ()))):
    return lax.dot_general(a, b, dims, preferred_element_type=f32)


def gather_grad(g_refs, g_scr, part, *, dp_count, mp_count, parts, piece_rows, tile_cols):
    for k, g_ref in enumerate(g_refs):
        piece = part - k
        at = pl.multiple_of(jnp.where(piece < 0, piece + parts, piece) * piece_rows, piece_rows)
        for o in range(dp_count):
            for m in range(mp_count):
                rows = pl.ds(o * parts * piece_rows + at, piece_rows)
                g_scr[rows, m * tile_cols : (m + 1) * tile_cols] = g_ref[o * mp_count + m]


def diagonal(shape, value):
    ids = lax.broadcasted_iota(jnp.int32, shape, 0)
    return jnp.where(ids == lax.broadcasted_iota(jnp.int32, shape, 1), value, 0.0)


def near_base_kernel(*refs, parts):
    s_refs, (out_ref, s_scr) = refs[:-2], refs[-2:]
    rows = s_refs[0].shape[1]
    half = rows * parts
    slot, part = lax.axis_index("mp") // parts, lax.axis_index("mp") % parts
    for k, s_ref in enumerate(s_refs):
        at = pl.multiple_of((part - k + parts) % parts * rows, rows)
        s_scr[:, pl.ds(at, rows), :] = s_ref[...]
    for g in range(2):

        @pl.when(slot == g)
        def _():
            mine = slice(g * half, (g + 1) * half)
            other = slice((1 - g) * half, (2 - g) * half)
            for side in range(2):
                square = decay_rate * s_scr[side, :, mine].astype(f32)
                out_ref[side, mine, mine] = square + diagonal((half, half), damping)
                across = decay_rate * s_scr[side, :, other].astype(f32)
                out_ref[side, mine, other] = across
                out_ref[side, other, mine] = across.T


def far_base_kernel(base_ref, *refs, parts):
    s_refs, (out_ref, s_scr) = refs[:-2], refs[-2:]
    rows, half = s_refs[0].shape[1:]
    slot, part = lax.axis_index("mp") // parts, lax.axis_index("mp") % parts
    for k, s_ref in enumerate(s_refs):
        at = pl.multiple_of((part - k + parts) % parts * rows, rows)
        s_scr[:, pl.ds(at, rows), :] = s_ref[...]
    for g in range(2):

        @pl.when(slot == g)
        def _():
            other = slice((1 - g) * half, (2 - g) * half)
            for side in range(2):
                square = decay_rate * s_scr[side].astype(f32)
                out_ref[side, other, other] = square + diagonal((half, half), damping)


def owner_kernel(*refs, n_g, split, sizes):
    g_refs, (base_ref, out_ref, g_scr, res_scr) = refs[:n_g], refs[n_g:]
    dp_count, mp_count, parts = sizes["dp_count"], sizes["mp_count"], sizes["parts"]
    piece_rows, tile_cols = sizes["piece_rows"], sizes["tile_cols"]
    order = g_scr.shape[0]
    part = lax.axis_index("mp") % parts
    if split:
        gather_grad(g_refs, g_scr, part, **sizes)
    else:
        g_scr[...] = g_refs[0][...]
    eye5 = diagonal((order, order), 5.0)
    grad = g_scr[...]
    bands = [slice(i, i + order // 2) for i in range(0, order, order // 2)]

    def factor_of(side):
        across = (((1 - side,), (1 - side,)), ((), ()))
        parts_of = []
        for at in bands:
            gram = dot(grad, grad[at] if side == 0 else grad[:, at], across)
            parts_of.append((base_ref[side, :, at] + (1.0 - decay_rate) * gram).astype(bf16))
        return jnp.concatenate(parts_of, axis=1)

    def moment_of(factor):
        norm = jnp.sum(jnp.square(factor.astype(f32)))
        return (2.5 / jnp.sqrt(norm) * factor.astype(f32)).astype(bf16)

    def step_of(moment):
        step = ((eye5 - moment.astype(f32)) * 0.25).astype(bf16)
        added = []
        for i in range(0, order, 128):
            block = slice(i, i + 128)
            exact = (diagonal((128, 128), 5.0) - moment[block, block].astype(f32)) * 0.25
            added.append(jnp.sum(step[block, block].astype(f32) - exact, axis=0, keepdims=True))
        return step, jnp.concatenate(added, axis=1)

    def partial_of(square, step, added):
        cube, partial_m, more = [], [], []
        for at in bands:
            power = dot(square, step[:, at])
            cube.append(power.astype(bf16))
            piece = square[:, at].astype(f32)
            partial_m.append((piece * (5.0 + 4.0 * added[:, at]) - 4.0 * power).astype(bf16))
            moment = jnp.sum(piece * partial_m[-1].astype(f32), axis=0, keepdims=True)
            rounded = ((5.0 - moment.astype(bf16).astype(f32)) * 0.25).astype(bf16)
            more.append(rounded.astype(f32) - (5.0 - moment) * 0.25)
        return [jnp.concatenate(x, axis=1) for x in (cube, partial_m, more)]

    def root_of(step, added, cube, partial_m):
        pieces = []
        for at in bands:
            last = dot(cube, partial_m[:, at])
            pieces.append((step[:, at].astype(f32) * (1.25 + added[:, at]) - 0.25 * last).astype(bf16))
        return jnp.concatenate(pieces, axis=1)

    def product(a, b):
        return dot(a, b).astype(bf16)

    factor = {1: factor_of(1), 0: factor_of(0)}
    step, added, square, cube, partial_m, root = {}, {}, {}, {}, {}, {}
    step[1], added[1] = step_of(moment_of(factor[1]))
    square[1] = product(step[1], step[1])
    step[0], added[0] = step_of(moment_of(factor[0]))
    cube[1], partial_m[1], added[1] = partial_of(square[1], step[1], added[1])
    square[0] = product(step[0], step[0])
    root[1] = root_of(step[1], added[1], cube[1], partial_m[1])
    cube[0], partial_m[0], added[0] = partial_of(square[0], step[0], added[0])
    grad_norm = jnp.sqrt(jnp.sum(jnp.square(grad.astype(f32))))
    right_applied = product(grad, root[1])
    root[0] = root_of(step[0], added[0], cube[0], partial_m[0])
    res_scr[...] = dot(root[0], right_applied).astype(bf16)
    scale = grad_norm / (jnp.sqrt(jnp.sum(jnp.square(res_scr[...].astype(f32)))) + 1e-06)
    if not split:
        out_ref[...] = (res_scr[...].astype(f32) * scale).astype(bf16)
        return
    at = pl.multiple_of(part * piece_rows, piece_rows)
    for o in range(dp_count):
        for m in range(mp_count):
            from_rows = pl.ds(o * parts * piece_rows + at, piece_rows)
            piece = res_scr[from_rows, m * tile_cols : (m + 1) * tile_cols].astype(f32)
            out_ref[o * mp_count + m] = (piece * scale).astype(bf16)


def stats_kernel(*refs, sizes):
    g_refs, (old_hbm, new_ref, g_scr, old_ref, sem) = refs[:-5], refs[-5:]
    parts = sizes["parts"]
    slots = sizes["mp_count"] // parts
    rows = old_ref.shape[2]
    old = pltpu.make_async_copy(old_hbm, old_ref, sem)
    old.start()
    my_index = lax.axis_index("mp")
    at = pl.multiple_of(my_index * rows, rows)
    for j in range(slots):
        gather_grad(g_refs[j * parts : (j + 1) * parts], g_scr.at[j], my_index % parts, **sizes)
        slot = (my_index // parts - j + slots) % slots
        left = dot(g_scr[j, pl.ds(at, rows), :], g_scr[j], (((1,), (1,)), ((), ())))
        right = dot(g_scr[j, :, pl.ds(at, rows)], g_scr[j], (((0,), (0,)), ((), ())))
        if j == 0:
            old.wait()
        new_ref[slot, 0] = decay_rate * old_ref[slot, 0] + (1.0 - decay_rate) * left
        new_ref[slot, 1] = decay_rate * old_ref[slot, 1] + (1.0 - decay_rate) * right


VMEM = pl.BlockSpec(memory_space=pltpu.VMEM)
SMEM = pl.BlockSpec(memory_space=pltpu.SMEM)
HBM = pl.BlockSpec(memory_space=pltpu.HBM)


def in_hbm(x):
    return pltpu.with_memory_space_constraint(x, pltpu.HBM)


def call(kernel, out_shape, in_specs, scratch=(), out_specs=VMEM, vmem=8, flops=0, aliases=None):
    return pl.pallas_call(
        kernel,
        out_shape=out_shape,
        in_specs=in_specs,
        out_specs=out_specs,
        scratch_shapes=list(scratch),
        input_output_aliases=aliases or {},
        compiler_params=pltpu.CompilerParams(vmem_limit_bytes=vmem * 2**20),
        cost_estimate=pl.CostEstimate(flops=flops, transcendentals=0, bytes_accessed=0) if flops else None,
    )


def step(grad_tiles, factor_stats, owner_blocks, rotation):
    dp_count = lax.axis_size("dp")
    mp_count = lax.axis_size("mp")
    tile_rows, tile_cols = grad_tiles.shape[1:]
    slots = owner_blocks.shape[1]
    rows, order = factor_stats.shape[2:]
    parts = mp_count // slots
    piece_rows = tile_rows // parts
    split = piece_rows % 16 == 0 and tile_cols % 128 == 0 and rows == tile_cols
    my_index = lax.axis_index("mp")
    my_slot = my_index // parts
    my_part = my_index % parts
    owners = owner_blocks.T
    where = dict(dp_count=dp_count, slots=slots)
    sizes = dict(
        dp_count=dp_count, mp_count=mp_count, parts=parts, piece_rows=piece_rows, tile_cols=tile_cols
    )
    table = pltpu.SMEM(owners.shape, jnp.int32)

    def to_slot(x, ahead):
        return lax.ppermute(x, "mp", [(i, (i + ahead * parts) % mp_count) for i in range(mp_count)])

    def to_part(x, ahead):
        return lax.ppermute(
            x, "mp", [(i, i // parts * parts + (i + ahead) % parts) for i in range(mp_count)]
        )

    def all_pieces(x):
        return [x] + [to_part(x, ahead) for ahead in range(1, parts)]

    def whole_grad(pieces):
        held = jnp.take(jnp.stack(pieces), (my_part - jnp.arange(parts)) % parts, axis=0)
        held = held.reshape(parts, dp_count, mp_count, piece_rows, tile_cols)
        return held.transpose(1, 0, 3, 2, 4).reshape(order, order)

    assert slots == 2
    half = rows * parts
    picked, far, near, table = call(
        functools.partial(pick_kernel, dp_count=dp_count, parts=parts),
        (
            pltpu.VMEM(grad_tiles.shape, bf16),
            pltpu.VMEM((2, rows, half), bf16),
            pltpu.VMEM((2, rows, order), bf16),
            pltpu.SMEM(owners.shape, jnp.int32),
        ),
        [HBM, SMEM, HBM, HBM],
        [
            pltpu.VMEM(grad_tiles.shape, bf16),
            pltpu.VMEM((2, rows, half), f32),
            pltpu.VMEM((2, rows, order), f32),
            pltpu.SemaphoreType.DMA((4,)),
        ],
        out_specs=(VMEM, VMEM, VMEM, SMEM),
    )(in_hbm(owners), rotation, in_hbm(grad_tiles), in_hbm(factor_stats))
    chunks = [near, to_slot(far, 1)]
    for ahead in range(1, parts):
        chunks.append(to_part(near, ahead))
        chunks.append(to_part(chunks[1], ahead))
    base_type = pltpu.VMEM((2, order, order), f32)
    base = call(
        functools.partial(near_base_kernel, parts=parts),
        base_type,
        [VMEM] * parts,
        [pltpu.VMEM((2, half, order), bf16)],
        flops=order**2,
    )(*chunks[0::2])
    base = call(
        functools.partial(far_base_kernel, parts=parts),
        base_type,
        [VMEM] * (parts + 1),
        [pltpu.VMEM((2, half, half), bf16)],
        flops=order**2,
        aliases={0: 0},
    )(base, *chunks[1::2])

    outgoing = picked.reshape(dp_count * mp_count, piece_rows, tile_cols)
    arrived = lax.all_to_all(outgoing, ("dp", "mp"), split_axis=0, concat_axis=0, tiled=True)
    pieces = all_pieces(arrived)
    theirs = [to_slot(arrived, ahead) for ahead in range(1, slots)]

    own_grad = pieces if split else [whole_grad(pieces)]
    result = call(
        functools.partial(owner_kernel, n_g=len(own_grad), split=split, sizes=sizes),
        pltpu.HBM(arrived.shape if split else (order, order), bf16),
        [VMEM] * (len(own_grad) + 1),
        [pltpu.VMEM((order, order), bf16), pltpu.VMEM((order, order), bf16)],
        vmem=24,
        flops=24 * order**3,
    )(*own_grad, base)
    if not split:
        result = result.reshape(dp_count, parts, piece_rows, mp_count, tile_cols)
        result = lax.dynamic_index_in_dim(result, my_part, 1, keepdims=False)
        result = result.transpose(0, 2, 1, 3).reshape(dp_count * mp_count, piece_rows, tile_cols)
    returned = lax.all_to_all(result, ("dp", "mp"), split_axis=0, concat_axis=0, tiled=True)

    grads = [pieces] + [all_pieces(x) for x in theirs]
    if split:
        new_stats = call(
            functools.partial(stats_kernel, sizes=sizes),
            jax.ShapeDtypeStruct(factor_stats.shape, f32),
            [VMEM] * (slots * parts) + [HBM],
            [
                pltpu.VMEM((slots, order, order), bf16),
                pltpu.VMEM(factor_stats.shape, f32),
                pltpu.SemaphoreType.DMA,
            ],
            vmem=16,
            flops=4 * slots * rows * order**2,
        )(*[x for slot_pieces in grads for x in slot_pieces], in_hbm(factor_stats))
    else:
        blocks = jnp.stack([whole_grad(x) for x in grads])
        blocks = jnp.take(blocks, (my_slot - jnp.arange(slots)) % slots, axis=0)
        row_part = lax.dynamic_slice_in_dim(blocks, my_index * rows, rows, 1)
        col_part = lax.dynamic_slice_in_dim(blocks, my_index * rows, rows, 2)
        left = jnp.einsum("kij,klj->kil", row_part, blocks, preferred_element_type=f32)
        right = jnp.einsum("kji,kjl->kil", col_part, blocks, preferred_element_type=f32)
        new_stats = decay_rate * factor_stats + (1.0 - decay_rate) * jnp.stack([left, right], axis=1)

    preconditioned = call(
        functools.partial(place_kernel, **where),
        jax.ShapeDtypeStruct(grad_tiles.shape, bf16),
        [SMEM, SMEM, VMEM],
        [pltpu.SemaphoreType.DMA((dp_count * slots,))],
        out_specs=HBM,
    )(table, rotation, returned.reshape(grad_tiles.shape))
    return (preconditioned, new_stats)


def solution(mesh):
    return placed(mesh)


def placed(mesh):
    return jax.shard_map(
        step,
        mesh=mesh,
        in_specs=(P(None, "dp", "mp"), P("dp", None, "mp", None), P(), P()),
        out_specs=(P(None, "dp", "mp"), P("dp", None, "mp", None)),
        check_vma=False,
    )
```

```python
import functools

import jax
import jax.numpy as jnp
from jax import lax
from jax.experimental import pallas as pl
from jax.experimental.pallas import tpu as pltpu
from jax.sharding import PartitionSpec as P


decay_rate = 0.9
damping = 1.0
bf16 = jnp.bfloat16
f32 = jnp.float32


def owner_of(owners_ref, rot, o, s, dp_count):
    row = o - rot
    return owners_ref[s, jnp.where(row < 0, row + dp_count, row)]


def each(count, one):
    lax.fori_loop(0, count, lambda j, carry: (one(j), carry)[1], 0, unroll=count <= 16)


def pick_kernel(
    owners_hbm, rot_ref, tiles_hbm, stats_hbm, out_ref, far_ref, near_ref, owners_ref, tiles_ref, far_scr, near_scr, sems,
    *, dp_count, parts
):
    slots = owners_ref.shape[0]
    half = far_scr.shape[2]
    slot = lax.axis_index("mp") // parts
    columns = pl.ds(pl.multiple_of(slot * half, half), half)
    pairs = (
        (owners_hbm, owners_ref),
        (tiles_hbm, tiles_ref),
        (stats_hbm.at[1 - slot, :, :, columns], far_scr),
        (stats_hbm.at[slot], near_scr),
    )
    copies = [pltpu.make_async_copy(a, b, sems.at[i]) for i, (a, b) in enumerate(pairs)]
    for copy in copies:
        copy.start()
    rot = rot_ref[0]
    copies[0].wait()
    copies[1].wait()

    def move(j):
        out_ref[j] = tiles_ref[owner_of(owners_ref, rot, j // slots, j % slots, dp_count)]

    each(dp_count * slots, move)
    copies[2].wait()
    far_ref[...] = far_scr[...].astype(bf16)
    copies[3].wait()
    near_ref[...] = near_scr[...].astype(bf16)


def place_kernel(owners_ref, rot_ref, in_ref, out_hbm, sems, *, dp_count, slots):
    rot = rot_ref[0]

    def copy(j):
        block = owner_of(owners_ref, rot, j // slots, j % slots, dp_count)
        return pltpu.make_async_copy(in_ref.at[j], out_hbm.at[block], sems.at[j])

    each(dp_count * slots, lambda j: copy(j).start())
    each(dp_count * slots, lambda j: copy(j).wait())


def dot(a, b, dims=(((1,), (0,)), ((), ()))):
    return lax.dot_general(a, b, dims, preferred_element_type=f32)


def gather_grad(g_refs, g_scr, part, *, dp_count, mp_count, parts, piece_rows, tile_cols):
    for k, g_ref in enumerate(g_refs):
        piece = part - k
        at = pl.multiple_of(jnp.where(piece < 0, piece + parts, piece) * piece_rows, piece_rows)
        for o in range(dp_count):
            for m in range(mp_count):
                rows = pl.ds(o * parts * piece_rows + at, piece_rows)
                g_scr[rows, m * tile_cols : (m + 1) * tile_cols] = g_ref[o * mp_count + m]


def diagonal(shape, value):
    ids = lax.broadcasted_iota(jnp.int32, shape, 0)
    return jnp.where(ids == lax.broadcasted_iota(jnp.int32, shape, 1), value, 0.0)


def near_base_kernel(*refs, parts):
    s_refs, (out_ref, s_scr) = refs[:-2], refs[-2:]
    rows = s_refs[0].shape[1]
    half = rows * parts
    slot, part = lax.axis_index("mp") // parts, lax.axis_index("mp") % parts
    for k, s_ref in enumerate(s_refs):
        at = pl.multiple_of((part - k + parts) % parts * rows, rows)
        s_scr[:, pl.ds(at, rows), :] = s_ref[...]
    for g in range(2):

        @pl.when(slot == g)
        def _():
            mine = slice(g * half, (g + 1) * half)
            other = slice((1 - g) * half, (2 - g) * half)
            for side in range(2):
                square = decay_rate * s_scr[side, :, mine].astype(f32)
                out_ref[side, mine, mine] = square + diagonal((half, half), damping)
                across = decay_rate * s_scr[side, :, other].astype(f32)
                out_ref[side, mine, other] = across
                out_ref[side, other, mine] = across.T


def far_base_kernel(base_ref, *refs, parts):
    s_refs, (out_ref, s_scr) = refs[:-2], refs[-2:]
    rows, half = s_refs[0].shape[1:]
    slot, part = lax.axis_index("mp") // parts, lax.axis_index("mp") % parts
    for k, s_ref in enumerate(s_refs):
        at = pl.multiple_of((part - k + parts) % parts * rows, rows)
        s_scr[:, pl.ds(at, rows), :] = s_ref[...]
    for g in range(2):

        @pl.when(slot == g)
        def _():
            other = slice((1 - g) * half, (2 - g) * half)
            for side in range(2):
                square = decay_rate * s_scr[side].astype(f32)
                out_ref[side, other, other] = square + diagonal((half, half), damping)


def owner_kernel(*refs, n_g, split, sizes):
    g_refs, (base_ref, out_ref, g_scr, res_scr) = refs[:n_g], refs[n_g:]
    dp_count, mp_count, parts = sizes["dp_count"], sizes["mp_count"], sizes["parts"]
    piece_rows, tile_cols = sizes["piece_rows"], sizes["tile_cols"]
    order = g_scr.shape[0]
    part = lax.axis_index("mp") % parts
    if split:
        gather_grad(g_refs, g_scr, part, **sizes)
    else:
        g_scr[...] = g_refs[0][...]
    eye5 = diagonal((order, order), 5.0)
    grad = g_scr[...]
    bands = [slice(i, i + order // 2) for i in range(0, order, order // 2)]

    def factor_of(side):
        across = (((1 - side,), (1 - side,)), ((), ()))
        parts_of = []
        for at in bands:
            gram = dot(grad, grad[at] if side == 0 else grad[:, at], across)
            parts_of.append((base_ref[side, :, at] + (1.0 - decay_rate) * gram).astype(bf16))
        return jnp.concatenate(parts_of, axis=1)

    def moment_of(factor):
        norm = jnp.sum(jnp.square(factor.astype(f32)))
        return (2.5 / jnp.sqrt(norm) * factor.astype(f32)).astype(bf16)

    def step_of(moment):
        step = ((eye5 - moment.astype(f32)) * 0.25).astype(bf16)
        added = []
        for i in range(0, order, 128):
            block = slice(i, i + 128)
            exact = (diagonal((128, 128), 5.0) - moment[block, block].astype(f32)) * 0.25
            added.append(jnp.sum(step[block, block].astype(f32) - exact, axis=0, keepdims=True))
        return step, jnp.concatenate(added, axis=1)

    def partial_of(square, step, added):
        cube, partial_m, more = [], [], []
        for at in bands:
            power = dot(square, step[:, at])
            cube.append(power.astype(bf16))
            piece = square[:, at].astype(f32)
            partial_m.append((piece * (5.0 + 4.0 * added[:, at]) - 4.0 * power).astype(bf16))
            moment = jnp.sum(piece * partial_m[-1].astype(f32), axis=0, keepdims=True)
            rounded = ((5.0 - moment.astype(bf16).astype(f32)) * 0.25).astype(bf16)
            more.append(rounded.astype(f32) - (5.0 - moment) * 0.25)
        return [jnp.concatenate(x, axis=1) for x in (cube, partial_m, more)]

    def root_of(step, added, cube, partial_m):
        pieces = []
        for at in bands:
            last = dot(cube, partial_m[:, at])
            pieces.append((step[:, at].astype(f32) * (1.25 + added[:, at]) - 0.25 * last).astype(bf16))
        return jnp.concatenate(pieces, axis=1)

    def product(a, b):
        return dot(a, b).astype(bf16)

    factor = {1: factor_of(1), 0: factor_of(0)}
    step, added, square, cube, partial_m, root = {}, {}, {}, {}, {}, {}
    step[1], added[1] = step_of(moment_of(factor[1]))
    square[1] = product(step[1], step[1])
    step[0], added[0] = step_of(moment_of(factor[0]))
    cube[1], partial_m[1], added[1] = partial_of(square[1], step[1], added[1])
    square[0] = product(step[0], step[0])
    root[1] = root_of(step[1], added[1], cube[1], partial_m[1])
    cube[0], partial_m[0], added[0] = partial_of(square[0], step[0], added[0])
    grad_norm = jnp.sqrt(jnp.sum(jnp.square(grad.astype(f32))))
    right_applied = product(grad, root[1])
    root[0] = root_of(step[0], added[0], cube[0], partial_m[0])
    squares = jnp.zeros((1, order // 2), f32)
    for at in bands:
        piece = dot(root[0], right_applied[:, at]).astype(bf16)
        res_scr[:, at] = piece
        squares += jnp.sum(jnp.square(piece.astype(f32)), axis=0, keepdims=True)
    scale = grad_norm / (jnp.sqrt(jnp.sum(squares)) + 1e-06)
    if not split:
        out_ref[...] = (res_scr[...].astype(f32) * scale).astype(bf16)
        return
    at = pl.multiple_of(part * piece_rows, piece_rows)
    for o in range(dp_count):
        for m in range(mp_count):
            from_rows = pl.ds(o * parts * piece_rows + at, piece_rows)
            piece = res_scr[from_rows, m * tile_cols : (m + 1) * tile_cols].astype(f32)
            out_ref[o * mp_count + m] = (piece * scale).astype(bf16)


def stats_kernel(*refs, sizes):
    g_refs, (old_hbm, new_ref, g_scr, old_ref, sem) = refs[:-5], refs[-5:]
    parts = sizes["parts"]
    slots = sizes["mp_count"] // parts
    rows = old_ref.shape[2]
    old = pltpu.make_async_copy(old_hbm, old_ref, sem)
    old.start()
    my_index = lax.axis_index("mp")
    at = pl.multiple_of(my_index * rows, rows)
    for j in range(slots):
        gather_grad(g_refs[j * parts : (j + 1) * parts], g_scr.at[j], my_index % parts, **sizes)
        slot = (my_index // parts - j + slots) % slots
        left = dot(g_scr[j, pl.ds(at, rows), :], g_scr[j], (((1,), (1,)), ((), ())))
        right = dot(g_scr[j, :, pl.ds(at, rows)], g_scr[j], (((0,), (0,)), ((), ())))
        if j == 0:
            old.wait()
        new_ref[slot, 0] = decay_rate * old_ref[slot, 0] + (1.0 - decay_rate) * left
        new_ref[slot, 1] = decay_rate * old_ref[slot, 1] + (1.0 - decay_rate) * right


VMEM = pl.BlockSpec(memory_space=pltpu.VMEM)
SMEM = pl.BlockSpec(memory_space=pltpu.SMEM)
HBM = pl.BlockSpec(memory_space=pltpu.HBM)


def in_hbm(x):
    return pltpu.with_memory_space_constraint(x, pltpu.HBM)


def call(kernel, out_shape, in_specs, scratch=(), out_specs=VMEM, vmem=8, flops=0, aliases=None):
    return pl.pallas_call(
        kernel,
        out_shape=out_shape,
        in_specs=in_specs,
        out_specs=out_specs,
        scratch_shapes=list(scratch),
        input_output_aliases=aliases or {},
        compiler_params=pltpu.CompilerParams(vmem_limit_bytes=vmem * 2**20),
        cost_estimate=pl.CostEstimate(flops=flops, transcendentals=0, bytes_accessed=0) if flops else None,
    )


def step(grad_tiles, factor_stats, owner_blocks, rotation):
    dp_count = lax.axis_size("dp")
    mp_count = lax.axis_size("mp")
    tile_rows, tile_cols = grad_tiles.shape[1:]
    slots = owner_blocks.shape[1]
    rows, order = factor_stats.shape[2:]
    parts = mp_count // slots
    piece_rows = tile_rows // parts
    split = piece_rows % 16 == 0 and tile_cols % 128 == 0 and rows == tile_cols
    my_index = lax.axis_index("mp")
    my_slot = my_index // parts
    my_part = my_index % parts
    owners = owner_blocks.T
    where = dict(dp_count=dp_count, slots=slots)
    sizes = dict(
        dp_count=dp_count, mp_count=mp_count, parts=parts, piece_rows=piece_rows, tile_cols=tile_cols
    )
    table = pltpu.SMEM(owners.shape, jnp.int32)

    def to_slot(x, ahead):
        return lax.ppermute(x, "mp", [(i, (i + ahead * parts) % mp_count) for i in range(mp_count)])

    def to_part(x, ahead):
        return lax.ppermute(
            x, "mp", [(i, i // parts * parts + (i + ahead) % parts) for i in range(mp_count)]
        )

    def all_pieces(x):
        return [x] + [to_part(x, ahead) for ahead in range(1, parts)]

    def whole_grad(pieces):
        held = jnp.take(jnp.stack(pieces), (my_part - jnp.arange(parts)) % parts, axis=0)
        held = held.reshape(parts, dp_count, mp_count, piece_rows, tile_cols)
        return held.transpose(1, 0, 3, 2, 4).reshape(order, order)

    assert slots == 2
    half = rows * parts
    picked, far, near, table = call(
        functools.partial(pick_kernel, dp_count=dp_count, parts=parts),
        (
            pltpu.VMEM(grad_tiles.shape, bf16),
            pltpu.VMEM((2, rows, half), bf16),
            pltpu.VMEM((2, rows, order), bf16),
            pltpu.SMEM(owners.shape, jnp.int32),
        ),
        [HBM, SMEM, HBM, HBM],
        [
            pltpu.VMEM(grad_tiles.shape, bf16),
            pltpu.VMEM((2, rows, half), f32),
            pltpu.VMEM((2, rows, order), f32),
            pltpu.SemaphoreType.DMA((4,)),
        ],
        out_specs=(VMEM, VMEM, VMEM, SMEM),
    )(in_hbm(owners), rotation, in_hbm(grad_tiles), in_hbm(factor_stats))
    chunks = [near, to_slot(far, 1)]
    for ahead in range(1, parts):
        chunks.append(to_part(near, ahead))
        chunks.append(to_part(chunks[1], ahead))
    base_type = pltpu.VMEM((2, order, order), f32)
    base = call(
        functools.partial(near_base_kernel, parts=parts),
        base_type,
        [VMEM] * parts,
        [pltpu.VMEM((2, half, order), bf16)],
        flops=order**2,
    )(*chunks[0::2])
    base = call(
        functools.partial(far_base_kernel, parts=parts),
        base_type,
        [VMEM] * (parts + 1),
        [pltpu.VMEM((2, half, half), bf16)],
        flops=order**2,
        aliases={0: 0},
    )(base, *chunks[1::2])

    outgoing = picked.reshape(dp_count * mp_count, piece_rows, tile_cols)
    arrived = lax.all_to_all(outgoing, ("dp", "mp"), split_axis=0, concat_axis=0, tiled=True)
    pieces = all_pieces(arrived)
    theirs = [to_slot(arrived, ahead) for ahead in range(1, slots)]

    own_grad = pieces if split else [whole_grad(pieces)]
    result = call(
        functools.partial(owner_kernel, n_g=len(own_grad), split=split, sizes=sizes),
        pltpu.HBM(arrived.shape if split else (order, order), bf16),
        [VMEM] * (len(own_grad) + 1),
        [pltpu.VMEM((order, order), bf16), pltpu.VMEM((order, order), bf16)],
        vmem=24,
        flops=24 * order**3,
    )(*own_grad, base)
    if not split:
        result = result.reshape(dp_count, parts, piece_rows, mp_count, tile_cols)
        result = lax.dynamic_index_in_dim(result, my_part, 1, keepdims=False)
        result = result.transpose(0, 2, 1, 3).reshape(dp_count * mp_count, piece_rows, tile_cols)
    returned = lax.all_to_all(result, ("dp", "mp"), split_axis=0, concat_axis=0, tiled=True)

    grads = [pieces] + [all_pieces(x) for x in theirs]
    if split:
        new_stats = call(
            functools.partial(stats_kernel, sizes=sizes),
            jax.ShapeDtypeStruct(factor_stats.shape, f32),
            [VMEM] * (slots * parts) + [HBM],
            [
                pltpu.VMEM((slots, order, order), bf16),
                pltpu.VMEM(factor_stats.shape, f32),
                pltpu.SemaphoreType.DMA,
            ],
            vmem=16,
            flops=4 * slots * rows * order**2,
        )(*[x for slot_pieces in grads for x in slot_pieces], in_hbm(factor_stats))
    else:
        blocks = jnp.stack([whole_grad(x) for x in grads])
        blocks = jnp.take(blocks, (my_slot - jnp.arange(slots)) % slots, axis=0)
        row_part = lax.dynamic_slice_in_dim(blocks, my_index * rows, rows, 1)
        col_part = lax.dynamic_slice_in_dim(blocks, my_index * rows, rows, 2)
        left = jnp.einsum("kij,klj->kil", row_part, blocks, preferred_element_type=f32)
        right = jnp.einsum("kji,kjl->kil", col_part, blocks, preferred_element_type=f32)
        new_stats = decay_rate * factor_stats + (1.0 - decay_rate) * jnp.stack([left, right], axis=1)

    preconditioned = call(
        functools.partial(place_kernel, **where),
        jax.ShapeDtypeStruct(grad_tiles.shape, bf16),
        [SMEM, SMEM, VMEM],
        [pltpu.SemaphoreType.DMA((dp_count * slots,))],
        out_specs=HBM,
    )(table, rotation, returned.reshape(grad_tiles.shape))
    return (preconditioned, new_stats)


def solution(mesh):
    return placed(mesh)


def placed(mesh):
    return jax.shard_map(
        step,
        mesh=mesh,
        in_specs=(P(None, "dp", "mp"), P("dp", None, "mp", None), P(), P()),
        out_specs=(P(None, "dp", "mp"), P("dp", None, "mp", None)),
        check_vma=False,
    )
```
